256 devices in a mesh: gx: 4 (over x), gy: 4 (over y_lo, core), gz: 16 (over z, y_hi).
Axes of the slice: x: 4, y: 4 (y_hi: 2, y_lo: 2; y = y_hi * 2 + y_lo), z: 8, core: 2. Of those that a mesh axis runs over, the one named last changes fastest.
Arguments:
- left_modes: bfloat16 [2, 4, 2, 128, 3, 131072], P(None, None, None, None, None, ('gx', 'gy', 'gz')), may hold values from -0.14160156 to 0.14160156
- right_modes: bfloat16 [2, 4, 2, 128, 3, 131072], P(None, None, None, None, None, ('gx', 'gy', 'gz')), may hold values from -0.14160156 to 0.14160156
- gamma_cols: int32 [16, 4], replicated, may hold values from 0 to 3, each once within a row
- gamma_phase: int32 [16, 4], replicated, may hold values from 0 to 3
- dilution: int32 [64], replicated, may hold values from 0 to 3
- time_pairs: int32 [4, 2], replicated, may hold values from 0 to 1
Outputs:
- meson_fields: float32 [16, 2, 2, 128, 128], P('gz', None, None, ('gx', 'gy'))
- traces: float32 [4, 16, 16, 2], P(None, 'gz')
The draws below stay inside these ranges and needn't reach their ends.
Inputs may be any that keep to these rules, and one draw needn't show every extreme that they name: Each row of gamma_cols is a permutation of the four spins.
All inputs are finite; a program needn't handle non-finite values.
Results may differ from the reference program's by a relative error of at most 0.0003.
Values sent between devices are 32-bit elements; how exact they have to be, the bound alone decides.
No kernel may reach another device: no remote copies, remote signals or barrier semaphores. Data moves between devices by JAX's collectives and lax.ppermute only.
A program may use at most 128 MiB of HBM per device.

```python
import math
import jax
import jax.numpy as jnp
from jax import lax

LOW = 64
NOISE = 64
N = 128
G = 16
TS = 2
NPAIR = 4
SITES = 131072


def touch_ends(array, own_key, least, high):
    dims = array.shape
    index_at = [jax.random.randint(jax.random.fold_in(own_key, axis), (), 0, dims[axis]) for axis in range(len(dims))]
    array = array.at[tuple(index_at)].set(least)
    longest = dims.index(max(dims))
    index_at[longest] = (index_at[longest] + 1) % dims[longest]
    return array.at[tuple(index_at)].set(high)


def level_of(rng, shape, split, low, top_value):
    def one(dim, parts):
        draws = jax.random.uniform(jax.random.fold_in(jax.random.fold_in(rng, 6), dim), (parts,), jnp.float32, low / len(split), top_value / len(split))
        return jnp.repeat(jnp.exp(draws), shape[dim] // parts).reshape((-1,) + (1,) * (len(shape) - dim - 1))

    loudness = one(*split[0])
    for cut in split[1:]:
        loudness = loudness * one(*cut)
    return loudness


def noise(key, extent, spread, limit, shards=(), kind=jnp.bfloat16):
    values = spread * jax.random.normal(key, extent, jnp.float32)
    if shards:
        values = values * level_of(key, extent, shards, -0.22, 0.18)
    return jnp.clip(values, -limit, limit).astype(kind)


def setup_inputs(seed: int = 0) -> dict:
    key_list = jax.random.split(jax.random.key(seed), 7)
    return {
        "left_modes": noise(key_list[0], (TS, 4, 2, N, 3, SITES), ((24 * SITES) ** -0.25), 0.14160156, ((5, 256),)),
        "right_modes": noise(key_list[1], (TS, 4, 2, N, 3, SITES), ((24 * SITES) ** -0.25), 0.14160156, ((5, 256),)),
        "gamma_cols": jax.vmap(lambda own: jax.random.permutation(own, 4))(jax.random.split(key_list[2], G)).reshape((G, 4)).astype(jnp.int32),
        "gamma_phase": touch_ends(jax.random.randint(key_list[3], (G, 4), 0, 4), jax.random.fold_in(key_list[3], 1), 0, 3).astype(jnp.int32),
        "dilution": touch_ends(jax.random.randint(key_list[4], (NOISE,), 0, 4), jax.random.fold_in(key_list[4], 1), 0, 3).astype(jnp.int32),
        "time_pairs": touch_ends(jax.random.randint(key_list[5], (NPAIR, 2), 0, TS), jax.random.fold_in(key_list[5], 1), 0, TS - 1).astype(jnp.int32),
    }


EXACT = lax.Precision.HIGHEST


def pair_products(left_slice, right_slice):
    block_size = math.gcd(left_slice.shape[-1], 4096)
    block_count = left_slice.shape[-1] // block_size

    def add_block(block_index, running):
        offset = (block_index * block_size).astype(jnp.int32)
        left_part = lax.dynamic_slice_in_dim(left_slice, offset, block_size, 4).astype(jnp.float32)
        right_part = lax.dynamic_slice_in_dim(right_slice, offset, block_size, 4).astype(jnp.float32)
        return running + jnp.einsum("spicx,qrjcx->sqpirj", left_part, right_part, precision=EXACT)

    zero_total = jnp.zeros((4, 4, 2, N, 2, N), jnp.float32)
    products = lax.fori_loop(0, block_count, add_block, zero_total)
    pair_re = products[:, :, 0, :, 0, :] + products[:, :, 1, :, 1, :]
    pair_im = products[:, :, 0, :, 1, :] - products[:, :, 1, :, 0, :]
    return pair_re, pair_im


def coefficients(gamma_cols, gamma_phase):
    spin_ids = jnp.arange(4, dtype=jnp.int32)
    onehot = (gamma_cols[:, :, None] == spin_ids[None, None, :]).astype(jnp.float32)
    real_sign = (gamma_phase == 0).astype(jnp.float32) - (gamma_phase == 2).astype(jnp.float32)
    imag_sign = (gamma_phase == 1).astype(jnp.float32) - (gamma_phase == 3).astype(jnp.float32)
    return onehot * real_sign[:, :, None], onehot * imag_sign[:, :, None]


def spin_mask(dilution):
    noise_spin = jnp.concatenate([jnp.full((LOW,), -1, jnp.int32), dilution.astype(jnp.int32)])
    spin_ids = jnp.arange(4, dtype=jnp.int32)
    keep_spin = (noise_spin[None, :] < 0) | (noise_spin[None, :] == spin_ids[:, None])
    return keep_spin.astype(jnp.float32)


def select_pairs(crossed, time_pairs):
    time_ids = jnp.arange(crossed.shape[1], dtype=jnp.int32)
    first_time = (time_pairs[:, 0:1] == time_ids[None, :]).astype(jnp.float32)
    second_time = (time_pairs[:, 1:2] == time_ids[None, :]).astype(jnp.float32)
    chosen = jnp.einsum("pt,pu,gtahub->pgahb", first_time, second_time, crossed, precision=EXACT)
    real_part = chosen[:, :, 0, :, 0] - chosen[:, :, 1, :, 1]
    imag_part = chosen[:, :, 0, :, 1] + chosen[:, :, 1, :, 0]
    return jnp.stack([real_part, imag_part], axis=-1)


def reference(left_modes, right_modes, gamma_cols, gamma_phase, dilution, time_pairs):
    mask_table = spin_mask(dilution)
    coef_re, coef_im = coefficients(gamma_cols, gamma_phase)
    real_list = []
    imag_list = []
    for time_slot in range(TS):
        pair_re, pair_im = pair_products(left_modes[time_slot], right_modes[time_slot])
        real_list.append(pair_re * mask_table[None, :, None, :])
        imag_list.append(pair_im * mask_table[None, :, None, :])
    pair_re = jnp.stack(real_list)
    pair_im = jnp.stack(imag_list)
    meson_re = jnp.einsum("gst,ustij->guij", coef_re, pair_re, precision=EXACT) - jnp.einsum("gst,ustij->guij", coef_im, pair_im, precision=EXACT)
    meson_im = jnp.einsum("gst,ustij->guij", coef_re, pair_im, precision=EXACT) + jnp.einsum("gst,ustij->guij", coef_im, pair_re, precision=EXACT)
    meson_fields = jnp.stack([meson_re, meson_im], axis=2)
    crossed = jnp.einsum("gtaij,hubji->gtahub", meson_fields, meson_fields, precision=EXACT)
    traces = select_pairs(crossed, time_pairs) / N
    return meson_fields, traces
```

```python
import functools

import jax
import jax.numpy as jnp
from jax import lax
from jax.experimental import pallas as pl
from jax.experimental.pallas import tpu as pltpu
from jax.sharding import PartitionSpec as P

AXES = ("gx", "gy", "gz")
EXACT = lax.Precision.HIGHEST
CHIPS = 128
ROWS = 20
VMEM = pltpu.MemorySpace.VMEM


def flat_index(chip, core):
    return (chip // 16) * 32 + core * 16 + chip % 16


CHIP_GROUPS = [[flat_index(chip, core) for chip in range(CHIPS)] for core in range(2)]
PARTNER = [(flat_index(chip, core), flat_index(chip, 1 - core)) for chip in range(CHIPS) for core in range(2)]


def lane_iota(shape):
    return lax.broadcasted_iota(jnp.int32, shape, len(shape) - 1)


def row_iota(shape):
    return lax.broadcasted_iota(jnp.int32, shape, len(shape) - 2)


def lane_swap(x, step):
    odd = (lane_iota(x.shape) & step) != 0
    return jnp.where(odd, pltpu.roll(x, step, 1), pltpu.roll(x, 128 - step, 1))


def lane_xor(x, amount, bits):
    for bit in bits:
        flip = ((amount >> bit) & 1) != 0
        x = jnp.where(flip, lane_swap(x, 1 << bit), x)
    return x


def products_kernel(slot_ref, left_ref, right_ref, pick_ref, out_ref, rows_ref):
    step = pl.program_id(0)

    @pl.when(step == 0)
    def _():
        for part in range(2):
            for colour in range(3):
                at = (part * 3 + colour) * 512
                noise = None
                for spin in range(4):
                    rows_ref[spin * 64 : spin * 64 + 64, at : at + 512] = right_ref[0, spin, part, colour, 0:64, :]
                    term = right_ref[0, spin, part, colour, 64:128, :] * pick_ref[spin]
                    noise = term if noise is None else noise + term
                rows_ref[256:320, at : at + 512] = noise

    cols = []
    for part in range(2):
        for colour in range(3):
            pieces = []
            for tile in range(2):
                lines = slice(tile * 16, tile * 16 + 16)
                for spin in range(4):
                    pieces.append(left_ref[0, spin, part, colour, lines, :])
                for spin in range(4):
                    other = left_ref[0, spin, 1 - part, colour, lines, :]
                    pieces.append(-other if part == 0 else other)
            cols.append(jnp.concatenate(pieces, axis=0))
    prod = lax.dot_general(
        rows_ref[...],
        jnp.concatenate(cols, axis=1),
        (((1,), (1,)), ((), ())),
        preferred_element_type=jnp.float32,
    )
    low_i = lane_iota((8, 128)) & 15
    within = row_iota((8, 128)) ^ (low_i & 7)
    upper = low_i >= 8
    for tile in range(2):
        i_high = step * 2 + tile
        for block in range(20):
            first = prod[block * 16 : block * 16 + 8, tile * 128 : tile * 128 + 128]
            second = prod[block * 16 + 8 : block * 16 + 16, tile * 128 : tile * 128 + 128]
            j_high = block % 4 if block < 16 else block - 12
            start = (i_high ^ j_high) * (16 * ROWS) + block
            low_half = jnp.take_along_axis(jnp.where(upper, second, first), within, axis=0)
            high_half = jnp.take_along_axis(jnp.where(upper, first, second), within, axis=0)
            out_ref[pl.ds(start, 8, stride=ROWS), :] = low_half
            out_ref[pl.ds(start + 8 * ROWS, 8, stride=ROWS), :] = high_half


def products(left, right, pick, slot):
    grid_spec = pltpu.PrefetchScalarGridSpec(
        num_scalar_prefetch=1,
        grid=(4,),
        in_specs=[
            pl.BlockSpec((1, 4, 2, 3, 32, 512), lambda n, slot: (slot[0], 0, 0, 0, n, 0)),
            pl.BlockSpec((1, 4, 2, 3, 128, 512), lambda n, slot: (slot[0], 0, 0, 0, 0, 0)),
            pl.BlockSpec((4, 64, 512), lambda n, slot: (0, 0, 0)),
        ],
        out_specs=pl.BlockSpec((CHIPS * ROWS, 128), lambda n, slot: (0, 0)),
        scratch_shapes=[pltpu.VMEM((320, 3072), jnp.bfloat16)],
    )
    return pl.pallas_call(
        products_kernel,
        grid_spec=grid_spec,
        out_shape=jax.ShapeDtypeStruct((CHIPS * ROWS, 128), jnp.float32),
        compiler_params=pltpu.CompilerParams(dimension_semantics=("arbitrary",)),
        name="products",
    )(slot, left, right, pick)


def sum_kernel(parts_ref, out_ref):
    def add(k, acc):
        return acc + parts_ref[pl.ds(pl.multiple_of(k * 40, 8), 40), :]

    both = lax.fori_loop(1, 64, add, parts_ref[0:40, :], unroll=7)
    out_ref[...] = both[0:20] + both[20:40]


def dot_exact(a, b, dims):
    return lax.dot_general(a, b, (dims, ((), ())), precision=EXACT, preferred_element_type=jnp.float32)


def combine_kernel(where_ref, own_ref, peer_ref, coef_ref, dil_ref, out_ref):
    chip = where_ref[0]
    core = where_ref[1]
    lane8 = lane_iota((8, 128))
    row8 = row_iota((8, 128))
    spin_of = lane_xor(dil_ref[...], chip & 15, range(4))
    noise_lane = lane8 >= 64
    fields = []
    for source in (own_ref, peer_ref):
        terms = []
        for spin in range(4):
            x = jnp.concatenate([source[spin * 4 : spin * 4 + 4, :], source[16:20, :]], axis=0)
            for level in range(3):
                row_bit = (row8 >> level) & 1
                lane_bit = (lane8 >> (level + 4)) & 1
                up = pltpu.roll(pltpu.roll(x, 1 << level, 0), 128 - (16 << level), 1)
                down = pltpu.roll(pltpu.roll(x, 8 - (1 << level), 0), 16 << level, 1)
                x = jnp.where(row_bit == lane_bit, x, jnp.where(row_bit == 1, up, down))
            keep = jnp.logical_or(jnp.logical_not(noise_lane), spin_of == spin)
            terms.append(jnp.where(keep, x, 0.0))
        fields.append(dot_exact(coef_ref[...], jnp.concatenate(terms, axis=0), ((1,), (0,))))
    mine, other = fields
    first = jnp.where(core == 0, mine, other)
    second = jnp.where(core == 0, other, mine)
    mirror = lane_xor(jnp.concatenate([first, second], axis=0), chip, range(7))
    cross = dot_exact(mine, mirror, ((1,), (1,)))
    zero = jnp.zeros((16, 64), jnp.float32)
    columns = []
    imag_columns = []
    for time in range(2):
        at = time * 32
        columns.append(cross[0:16, at : at + 16] - cross[16:32, at + 16 : at + 32])
        columns.append(cross[0:16, at + 16 : at + 32] + cross[16:32, at : at + 16])
    trace_rows = jnp.concatenate(columns + [zero], axis=1)
    ordered = lane_xor(mine, chip & 112, range(4, 7))
    lane = lane_iota((16, 128))
    for block in range(16):
        real = pltpu.roll(ordered[0:16], (64 - 8 * block) % 128, 1)
        imag = pltpu.roll(ordered[16:32], (72 - 8 * block) % 128, 1)
        rows = jnp.where(lane < 64, trace_rows, jnp.where(lane < 72, real, jnp.where(lane < 80, imag, 0.0)))
        out_ref[block * 16 : block * 16 + 16, :] = rows


def finish_kernel(where_ref, pairs_ref, got_ref, fields_ref, traces_ref):
    block = where_ref[2]
    lane = lane_iota((16, 128))
    row = row_iota((16, 128))
    sums = []
    for time in range(2):
        pieces = [got_ref[(k * 2 + time) * 16 : (k * 2 + time) * 16 + 16, :] for k in range(8)]
        total = pieces[0]
        for piece in pieces[1:]:
            total = total + piece
        sums.append(jnp.sum(total, axis=0, keepdims=True))
        by_chip = jnp.transpose(jnp.concatenate(pieces, axis=0))[64:80, :]
        x = lane_xor(by_chip, block * 8, range(3, 7))
        for bit in range(3):
            x = jnp.where(((row >> bit) & 1) != 0, lane_swap(x, 1 << bit), x)
        fields_ref[0, time, 0] = x[0:8]
        fields_ref[0, time, 1] = x[8:16]
    for pair in range(4):
        first = jnp.where(pairs_ref[pair, 0] == 0, sums[0], sums[1])
        picked = jnp.where(pairs_ref[pair, 1] == 0, first[:, 0:32], first[:, 32:64])
        traces_ref[pair : pair + 1, :] = picked / 128.0


def coefficients(gamma_cols, gamma_phase):
    spin_ids = jnp.arange(4, dtype=jnp.int32)
    onehot = (gamma_cols[:, :, None] == spin_ids[None, None, :]).astype(jnp.float32)
    real_sign = (gamma_phase == 0).astype(jnp.float32) - (gamma_phase == 2).astype(jnp.float32)
    imag_sign = (gamma_phase == 1).astype(jnp.float32) - (gamma_phase == 3).astype(jnp.float32)
    real = (onehot * real_sign[:, :, None]).transpose(0, 2, 1)
    imag = (onehot * imag_sign[:, :, None]).transpose(0, 2, 1)
    top = jnp.stack([real, -imag], axis=2)
    bottom = jnp.stack([imag, real], axis=2)
    return jnp.stack([top, bottom]).reshape(32, 32)


def whole(shape):
    return pl.BlockSpec(shape, lambda *_: (0,) * len(shape), memory_space=VMEM)


SMEM = pl.BlockSpec(memory_space=pltpu.MemorySpace.SMEM)


def local(left_modes, right_modes, gamma_cols, gamma_phase, dilution, time_pairs):
    gx, gy, gz = (lax.axis_index(name) for name in AXES)
    core = gy % 2
    chip = (gx * 2 + gy // 2) * 16 + gz
    where = jnp.stack([chip, core, gx * 4 + gy]).astype(jnp.int32)
    left = jnp.transpose(left_modes, (0, 1, 2, 4, 3, 5))
    right = jnp.transpose(right_modes, (0, 1, 2, 4, 3, 5))
    pick = (dilution[None, :] == jnp.arange(4, dtype=jnp.int32)[:, None]).astype(jnp.bfloat16)
    pick = jnp.broadcast_to(pick[:, :, None], (4, 64, 512))
    coef = coefficients(gamma_cols, gamma_phase)
    dil = jnp.broadcast_to(jnp.concatenate([dilution, dilution])[None, :], (8, 128))

    away = products(left, right, pick, (1 - core)[None].astype(jnp.int32))
    arrived = lax.ppermute(away, AXES, PARTNER)
    home = products(left, right, pick, core[None].astype(jnp.int32))
    partial = (home + arrived).reshape(CHIPS * 5, 4, 128)
    parts = lax.all_to_all(partial, AXES, 0, 0, axis_index_groups=CHIP_GROUPS, tiled=True)
    own = pl.pallas_call(
        sum_kernel,
        in_specs=[whole((CHIPS * ROWS, 128))],
        out_specs=whole((ROWS, 128)),
        out_shape=jax.ShapeDtypeStruct((ROWS, 128), jnp.float32),
        name="sum_parts",
    )(parts.reshape(CHIPS * ROWS, 128))
    peer = lax.ppermute(own, AXES, PARTNER)
    rows = pl.pallas_call(
        combine_kernel,
        in_specs=[SMEM, whole((ROWS, 128)), whole((ROWS, 128)), whole((32, 32)), whole((8, 128))],
        out_specs=whole((256, 128)),
        out_shape=jax.ShapeDtypeStruct((256, 128), jnp.float32),
        name="combine",
    )(where, own, peer, coef, dil)
    got = lax.all_to_all(rows, AXES, 0, 0, tiled=True)
    fields, traces = pl.pallas_call(
        finish_kernel,
        in_specs=[SMEM, SMEM, whole((256, 128))],
        out_specs=[whole((1, 2, 2, 8, 128)), whole((4, 32))],
        out_shape=[
            jax.ShapeDtypeStruct((1, 2, 2, 8, 128), jnp.float32),
            jax.ShapeDtypeStruct((4, 32), jnp.float32),
        ],
        name="finish",
    )(where, time_pairs, got)
    traces = traces.reshape(4, 1, 2, 16).transpose(0, 1, 3, 2)
    return (fields, traces)


def solution(mesh):
    return jax.shard_map(
        local,
        mesh=mesh,
        in_specs=(
            P(None, None, None, None, None, AXES),
            P(None, None, None, None, None, AXES),
            P(),
            P(),
            P(),
            P(),
        ),
        out_specs=(P("gz", None, None, ("gx", "gy"), None), P(None, "gz", None, None)),
        check_vma=False,
    )
```

```python
import jax
import jax.numpy as jnp
from jax import lax
from jax.experimental import pallas as pl
from jax.experimental.pallas import tpu as pltpu
from jax.sharding import PartitionSpec as P

AXES = ("gx", "gy", "gz")
EXACT = lax.Precision.HIGHEST
CHIPS = 128
ROWS = 20
VMEM = pltpu.MemorySpace.VMEM


def flat_index(chip, core):
    return (chip // 16) * 32 + core * 16 + (chip % 8) * 2 + (chip // 8) % 2


PLANES = [[flat_index(plane * 8 + z, core) for plane in range(16)] for z in range(8) for core in range(2)]
COLUMNS = [[flat_index(plane * 8 + z, core) for z in range(8)] for plane in range(16) for core in range(2)]
PARTNER = [(flat_index(chip, core), flat_index(chip, 1 - core)) for chip in range(CHIPS) for core in range(2)]


def lane_iota(shape):
    return lax.broadcasted_iota(jnp.int32, shape, len(shape) - 1)


def row_iota(shape):
    return lax.broadcasted_iota(jnp.int32, shape, len(shape) - 2)


def lane_swap(x, step):
    odd = (lane_iota(x.shape) & step) != 0
    return jnp.where(odd, pltpu.roll(x, step, 1), pltpu.roll(x, 128 - step, 1))


def lane_xor(x, amount, bits):
    for bit in bits:
        flip = ((amount >> bit) & 1) != 0
        x = jnp.where(flip, lane_swap(x, 1 << bit), x)
    return x


def products_kernel(slot_ref, left_ref, right_ref, dil_ref, out_ref, rows_ref):
    step = pl.program_id(0)

    @pl.when(step == 0)
    def _():
        dilution = jnp.broadcast_to(jnp.concatenate([dil_ref[...], dil_ref[...]], axis=1), (128, 128))
        spin_of = jnp.transpose(dilution)[0:64, :]
        pick = []
        for spin in range(4):
            one = jnp.where(spin_of == spin, 1.0, 0.0).astype(jnp.bfloat16)
            pick.append(jnp.concatenate([one] * 4, axis=1))
        for part in range(2):
            for colour in range(3):
                at = (part * 3 + colour) * 512
                noise = None
                for spin in range(4):
                    rows_ref[spin * 64 : spin * 64 + 64, at : at + 512] = right_ref[0, spin, part, colour, 0:64, :]
                    term = right_ref[0, spin, part, colour, 64:128, :] * pick[spin]
                    noise = term if noise is None else noise + term
                rows_ref[256:320, at : at + 512] = noise

    cols = []
    for part in range(2):
        for colour in range(3):
            pieces = []
            for tile in range(2):
                lines = slice(tile * 16, tile * 16 + 16)
                for spin in range(4):
                    pieces.append(left_ref[0, spin, part, colour, lines, :])
                for spin in range(4):
                    other = left_ref[0, spin, 1 - part, colour, lines, :]
                    pieces.append(-other if part == 0 else other)
            cols.append(jnp.concatenate(pieces, axis=0))
    prod = lax.dot_general(
        rows_ref[...],
        jnp.concatenate(cols, axis=1),
        (((1,), (1,)), ((), ())),
        preferred_element_type=jnp.float32,
    )
    low_i = lane_iota((8, 128)) & 15
    within = row_iota((8, 128)) ^ (low_i & 7)
    upper = low_i >= 8
    for tile in range(2):
        i_high = step * 2 + tile
        for block in range(20):
            first = prod[block * 16 : block * 16 + 8, tile * 128 : tile * 128 + 128]
            second = prod[block * 16 + 8 : block * 16 + 16, tile * 128 : tile * 128 + 128]
            j_high = block % 4 if block < 16 else block - 12
            start = (i_high ^ j_high) * (16 * ROWS) + block
            low_half = jnp.take_along_axis(jnp.where(upper, second, first), within, axis=0)
            high_half = jnp.take_along_axis(jnp.where(upper, first, second), within, axis=0)
            out_ref[pl.ds(start, 8, stride=ROWS), :] = low_half
            out_ref[pl.ds(start + 8 * ROWS, 8, stride=ROWS), :] = high_half


def products(left, right, dil, slot):
    grid_spec = pltpu.PrefetchScalarGridSpec(
        num_scalar_prefetch=1,
        grid=(4,),
        in_specs=[
            pl.BlockSpec((1, 4, 2, 3, 32, 512), lambda n, slot: (slot[0], 0, 0, 0, n, 0)),
            pl.BlockSpec((1, 4, 2, 3, 128, 512), lambda n, slot: (slot[0], 0, 0, 0, 0, 0)),
            pl.BlockSpec((1, 64), lambda n, slot: (0, 0)),
        ],
        out_specs=pl.BlockSpec(memory_space=VMEM),
        scratch_shapes=[pltpu.VMEM((320, 3072), jnp.bfloat16)],
    )
    return pl.pallas_call(
        products_kernel,
        grid_spec=grid_spec,
        out_shape=pltpu.VMEM((CHIPS * ROWS, 128), jnp.float32),
        compiler_params=pltpu.CompilerParams(dimension_semantics=("arbitrary",)),
        name="products",
    )(slot, left, right, dil)


def place():
    gx, gy, gz = (lax.axis_index(name) for name in AXES)
    chip = gx * 32 + (gy >> 1) * 16 + (gz & 1) * 8 + (gz >> 1)
    return chip, gy & 1, gx * 4 + gy


def sum_planes_kernel(parts_ref, out_ref):
    total = parts_ref[0:160, :]
    for k in range(1, 16):
        total = total + parts_ref[k * 160 : k * 160 + 160, :]
    out_ref[...] = total


def sum_columns_kernel(parts_ref, out_ref):
    both = parts_ref[0:40, :]
    for k in range(1, 4):
        both = both + parts_ref[k * 40 : k * 40 + 40, :]
    out_ref[...] = both[0:20] + both[20:40]


def dot_exact(a, b, dims):
    return lax.dot_general(a, b, (dims, ((), ())), precision=EXACT, preferred_element_type=jnp.float32)


def combine_kernel(own_ref, peer_ref, cols_ref, phase_ref, dil_ref, out_ref):
    chip, core, _ = place()
    coef = coefficients(cols_ref[...], phase_ref[...])
    lane8 = lane_iota((8, 128))
    row8 = row_iota((8, 128))
    dilution = jnp.broadcast_to(jnp.concatenate([dil_ref[...], dil_ref[...]], axis=1), (8, 128))
    spin_of = lane_xor(dilution, chip & 15, range(4))
    noise_lane = lane8 >= 64
    fields = []
    for source in (own_ref, peer_ref):
        terms = []
        for spin in range(4):
            x = jnp.concatenate([source[spin * 4 : spin * 4 + 4, :], source[16:20, :]], axis=0)
            for level in range(3):
                row_bit = (row8 >> level) & 1
                lane_bit = (lane8 >> (level + 4)) & 1
                up = pltpu.roll(pltpu.roll(x, 1 << level, 0), 128 - (16 << level), 1)
                down = pltpu.roll(pltpu.roll(x, 8 - (1 << level), 0), 16 << level, 1)
                x = jnp.where(row_bit == lane_bit, x, jnp.where(row_bit == 1, up, down))
            keep = jnp.logical_or(jnp.logical_not(noise_lane), spin_of == spin)
            terms.append(jnp.where(keep, x, 0.0))
        fields.append(dot_exact(coef, jnp.concatenate(terms, axis=0), ((0,), (0,))))
    mine, other = fields
    first = jnp.where(core == 0, mine, other)
    second = jnp.where(core == 0, other, mine)
    mirror = lane_xor(jnp.concatenate([first, second], axis=0), chip, range(7))
    cross = dot_exact(mine, mirror, ((1,), (1,)))
    zero = jnp.zeros((16, 64), jnp.float32)
    columns = []
    imag_columns = []
    for time in range(2):
        at = time * 32
        columns.append(cross[0:16, at : at + 16] - cross[16:32, at + 16 : at + 32])
        columns.append(cross[0:16, at + 16 : at + 32] + cross[16:32, at : at + 16])
    trace_rows = jnp.concatenate(columns + [zero], axis=1)
    ordered = lane_xor(mine, chip & 112, range(4, 7))
    lane = lane_iota((16, 128))
    for block in range(16):
        real = pltpu.roll(ordered[0:16], (64 - 8 * block) % 128, 1)
        imag = pltpu.roll(ordered[16:32], (72 - 8 * block) % 128, 1)
        rows = jnp.where(lane < 64, trace_rows, jnp.where(lane < 72, real, jnp.where(lane < 80, imag, 0.0)))
        out_ref[block * 16 : block * 16 + 16, :] = rows


def finish_kernel(pairs_ref, got_ref, fields_ref, traces_ref):
    _, _, block = place()
    row = row_iota((16, 128))
    sums = []
    for time in range(2):
        pieces = []
        for k in range(8):
            for high in range(2):
                pieces.append(got_ref[pl.ds((k * 2 + time) * 16 + high, 8, stride=2), :])
        total = pieces[0]
        for piece in pieces[1:]:
            total = total + piece
        sums.append(jnp.sum(total, axis=0, keepdims=True))
        by_chip = jnp.transpose(jnp.concatenate(pieces, axis=0))[64:80, :]
        x = lane_xor(by_chip, block * 8, range(3, 7))
        for bit in range(3):
            x = jnp.where(((row >> bit) & 1) != 0, lane_swap(x, 1 << bit), x)
        fields_ref[0, time, 0] = x[0:8]
        fields_ref[0, time, 1] = x[8:16]
    for pair in range(4):
        first = jnp.where(pairs_ref[pair, 0] == 0, sums[0], sums[1])
        picked = jnp.where(pairs_ref[pair, 1] == 0, first[:, 0:32], first[:, 32:64]) / 128.0
        traces_ref[pair, 0, 0:1, :] = picked[:, 0:16]
        traces_ref[pair, 0, 1:2, :] = picked[:, 16:32]


def coefficients(cols, phase):
    real = jnp.where(phase == 0, 1.0, jnp.where(phase == 2, -1.0, 0.0))
    imag = jnp.where(phase == 1, 1.0, jnp.where(phase == 3, -1.0, 0.0))
    blocks = []
    for spin in range(4):
        here = jnp.where(cols == spin, 1.0, 0.0)
        blocks.append(jnp.concatenate([here * real, here * imag], axis=1))
        blocks.append(jnp.concatenate([-here * imag, here * real], axis=1))
    return jnp.concatenate(blocks, axis=0)


def in_vmem(x):
    return pltpu.with_memory_space_constraint(x, VMEM)


VMEM_SPEC = pl.BlockSpec(memory_space=VMEM)
SMEM_SPEC = pl.BlockSpec(memory_space=pltpu.MemorySpace.SMEM)


def call(kernel, name, out_shape, *operands, specs=None):
    return pl.pallas_call(
        kernel,
        in_specs=specs or [VMEM_SPEC] * len(operands),
        out_specs=jax.tree.map(lambda _: VMEM_SPEC, out_shape),
        out_shape=out_shape,
        name=name,
    )(*operands)


def local(left_modes, right_modes, gamma_cols, gamma_phase, dilution, time_pairs):
    core = lax.axis_index("gy") % 2
    left = jnp.transpose(left_modes, (0, 1, 2, 4, 3, 5))
    right = jnp.transpose(right_modes, (0, 1, 2, 4, 3, 5))
    dil = dilution.reshape(1, 64)

    away = products(left, right, dil, (1 - core)[None].astype(jnp.int32))
    arrived = lax.ppermute(away, AXES, PARTNER)
    home = products(left, right, dil, core[None].astype(jnp.int32))
    partial = (home + arrived).reshape(16, 160, 128)
    parts = lax.all_to_all(partial, AXES, 0, 0, axis_index_groups=PLANES, tiled=True)
    plane = call(sum_planes_kernel, "sum_planes", pltpu.VMEM((160, 128), jnp.float32), in_vmem(parts.reshape(2560, 128)))
    parts = lax.all_to_all(plane.reshape(8, 1, 2560), AXES, 0, 0, axis_index_groups=COLUMNS, tiled=True)
    own = call(sum_columns_kernel, "sum_columns", pltpu.VMEM((ROWS, 128), jnp.float32), in_vmem(parts.reshape(160, 128)))
    peer = lax.ppermute(own, AXES, PARTNER)
    rows = call(
        combine_kernel,
        "combine",
        pltpu.VMEM((256, 128), jnp.float32),
        in_vmem(own),
        in_vmem(peer),
        in_vmem(gamma_cols.T),
        in_vmem(gamma_phase.T),
        in_vmem(dil),
    )
    got = lax.all_to_all(rows.reshape(256, 1, 128), AXES, 0, 0, tiled=True)
    fields, traces = pl.pallas_call(
        finish_kernel,
        in_specs=[SMEM_SPEC, VMEM_SPEC],
        out_specs=[VMEM_SPEC, VMEM_SPEC],
        out_shape=[
            jax.ShapeDtypeStruct((1, 2, 2, 8, 128), jnp.float32),
            jax.ShapeDtypeStruct((4, 1, 2, 16), jnp.float32),
        ],
        name="finish",
    )(time_pairs, in_vmem(got.reshape(256, 128)))
    return (fields, jnp.swapaxes(traces, 2, 3))


def solution(mesh):
    return jax.shard_map(
        local,
        mesh=mesh,
        in_specs=(
            P(None, None, None, None, None, AXES),
            P(None, None, None, None, None, AXES),
            P(),
            P(),
            P(),
            P(),
        ),
        out_specs=(P("gz", None, None, ("gx", "gy"), None), P(None, "gz", None, None)),
        check_vma=False,
    )
```

```python
import jax
import jax.numpy as jnp
from jax import lax
from jax.experimental import pallas as pl
from jax.experimental.pallas import tpu as pltpu
from jax.sharding import PartitionSpec as P

AXES = ("gx", "gy", "gz")
EXACT = lax.Precision.HIGHEST
CHIPS = 128
ROWS = 20
VMEM = pltpu.MemorySpace.VMEM


def flat_index(chip, core):
    bit = [(chip >> k) & 1 for k in range(7)]
    return bit[6] * 128 + bit[4] * 64 + bit[3] * 32 + core * 16 + (chip % 8) * 2 + bit[5]


PLANES = [[flat_index(plane * 8 + z, core) for plane in range(16)] for z in range(8) for core in range(2)]
COLUMNS = [[flat_index(plane * 8 + z, core) for z in range(8) for core in range(2)] for plane in range(16)]
PARTNER = [(flat_index(chip, core), flat_index(chip, 1 - core)) for chip in range(CHIPS) for core in range(2)]
SAME_CORE = [sorted(flat_index(chip, core) for chip in range(CHIPS)) for core in range(2)]


def lane_iota(shape):
    return lax.broadcasted_iota(jnp.int32, shape, len(shape) - 1)


def row_iota(shape):
    return lax.broadcasted_iota(jnp.int32, shape, len(shape) - 2)


def lane_swap(x, step):
    odd = (lane_iota(x.shape) & step) != 0
    return jnp.where(odd, pltpu.roll(x, step, 1), pltpu.roll(x, 128 - step, 1))


def lane_xor(x, amount, bits):
    for bit in bits:
        flip = ((amount >> bit) & 1) != 0
        x = jnp.where(flip, lane_swap(x, 1 << bit), x)
    return x


def place():
    gx, gy, gz = (lax.axis_index(name) for name in AXES)
    chip = (gx >> 1) * 64 + (gz & 1) * 32 + (gx & 1) * 16 + (gy >> 1) * 8 + (gz >> 1)
    return chip, gy & 1, gx * 4 + gy


def fill_rows(right_ref, dil_ref, rows_ref):
    dilution = jnp.broadcast_to(jnp.concatenate([dil_ref[...], dil_ref[...]], axis=1), (128, 128))
    spin_of = jnp.transpose(dilution)[0:64, :]
    pick = []
    for spin in range(4):
        one = jnp.where(spin_of == spin, 1.0, 0.0).astype(jnp.bfloat16)
        pick.append(jnp.concatenate([one] * 4, axis=1))
    for part in range(2):
        for colour in range(3):
            at = (part * 3 + colour) * 512
            noise = None
            for spin in range(4):
                rows_ref[spin * 64 : spin * 64 + 64, at : at + 512] = right_ref[spin, part, colour, 0:64, :]
                term = right_ref[spin, part, colour, 64:128, :] * pick[spin]
                noise = term if noise is None else noise + term
            rows_ref[256:320, at : at + 512] = noise


def add_tile(step, left_ref, rows_ref, out_ref):
    cols = []
    for part in range(2):
        for colour in range(3):
            pieces = []
            for tile in range(2):
                lines = slice(step * 32 + tile * 16, step * 32 + tile * 16 + 16)
                for spin in range(4):
                    pieces.append(left_ref[spin, part, colour, lines, :])
                for spin in range(4):
                    other = left_ref[spin, 1 - part, colour, lines, :]
                    pieces.append(-other if part == 0 else other)
            cols.append(jnp.concatenate(pieces, axis=0))
    prod = lax.dot_general(
        rows_ref[...],
        jnp.concatenate(cols, axis=1),
        (((1,), (1,)), ((), ())),
        preferred_element_type=jnp.float32,
    )
    low_i = lane_iota((8, 128)) & 15
    within = row_iota((8, 128)) ^ (low_i & 7)
    upper = low_i >= 8
    for tile in range(2):
        i_high = step * 2 + tile
        for block in range(20):
            first = prod[block * 16 : block * 16 + 8, tile * 128 : tile * 128 + 128]
            second = prod[block * 16 + 8 : block * 16 + 16, tile * 128 : tile * 128 + 128]
            j_high = block % 4 if block < 16 else block - 12
            start = (i_high ^ j_high) * (16 * ROWS) + block
            low_half = jnp.take_along_axis(jnp.where(upper, second, first), within, axis=0)
            high_half = jnp.take_along_axis(jnp.where(upper, first, second), within, axis=0)
            out_ref[pl.ds(start, 8, stride=ROWS), :] = low_half
            out_ref[pl.ds(start + 8 * ROWS, 8, stride=ROWS), :] = high_half


def away_kernel(left_ref, right_ref, dil_ref, out_ref, next_left_ref, next_right_ref, rows_ref, left_buf, right_buf, sems):
    _, core, _ = place()
    right_copies = [
        pltpu.make_async_copy(right_ref.at[1 - core, spin], right_buf.at[spin], sems.at[spin]) for spin in range(4)
    ]
    left_copies = []
    for step in range(4):
        lines = pl.ds(step * 32, 32)
        left_copies.append(
            pltpu.make_async_copy(
                left_ref.at[1 - core, :, :, :, lines, :], left_buf.at[:, :, :, lines, :], sems.at[4 + step]
            )
        )
    next_copies = [
        pltpu.make_async_copy(right_ref.at[core], next_right_ref, sems.at[8]),
        pltpu.make_async_copy(left_ref.at[core], next_left_ref, sems.at[9]),
    ]
    for copy in right_copies + left_copies:
        copy.start()
    for copy in right_copies:
        copy.wait()
    for copy in next_copies:
        copy.start()
    fill_rows(right_buf, dil_ref, rows_ref)
    for step in range(4):
        left_copies[step].wait()
        add_tile(step, left_buf, rows_ref, out_ref)
    for copy in next_copies:
        copy.wait()


def home_kernel(left_ref, right_ref, dil_ref, out_ref, rows_ref):
    fill_rows(right_ref, dil_ref, rows_ref)
    for step in range(4):
        add_tile(step, left_ref, rows_ref, out_ref)


def products(left, right, dil):
    slot = (4, 2, 3, 128, 512)
    rows = pltpu.VMEM((320, 3072), jnp.bfloat16)
    whole = pltpu.VMEM((CHIPS * ROWS, 128), jnp.float32)
    away, next_left, next_right = pl.pallas_call(
        away_kernel,
        in_specs=[HBM_SPEC, HBM_SPEC, VMEM_SPEC],
        out_specs=[VMEM_SPEC] * 3,
        out_shape=[whole, pltpu.VMEM(slot, jnp.bfloat16), pltpu.VMEM(slot, jnp.bfloat16)],
        scratch_shapes=[
            rows,
            pltpu.VMEM(slot, jnp.bfloat16),
            pltpu.VMEM(slot, jnp.bfloat16),
            pltpu.SemaphoreType.DMA((10,)),
        ],
        compiler_params=pltpu.CompilerParams(vmem_limit_bytes=16 << 20),
        name="away",
    )(*(pltpu.with_memory_space_constraint(x, pltpu.MemorySpace.HBM) for x in (left, right)), dil)
    arrived = lax.ppermute(away, AXES, PARTNER)
    home = pl.pallas_call(
        home_kernel,
        in_specs=[VMEM_SPEC] * 3,
        out_specs=VMEM_SPEC,
        out_shape=whole,
        scratch_shapes=[rows],
        compiler_params=pltpu.CompilerParams(vmem_limit_bytes=12 << 20),
        name="home",
    )(in_vmem(next_left), in_vmem(next_right), dil)
    return call(add_kernel, "add", whole, in_vmem(home), in_vmem(arrived))


def add_kernel(a_ref, b_ref, out_ref):
    out_ref[...] = a_ref[...] + b_ref[...]


def sum_planes_kernel(parts_ref, out_ref):
    total = parts_ref[0:160, :]
    for k in range(1, 16):
        total = total + parts_ref[k * 160 : k * 160 + 160, :]
    for z in range(8):
        mine = total[z * ROWS : z * ROWS + ROWS]
        out_ref[z * 40 : z * 40 + 40, :] = jnp.concatenate([mine, mine], axis=0)


def dot_exact(a, b, dims):
    return lax.dot_general(a, b, (dims, ((), ())), precision=EXACT, preferred_element_type=jnp.float32)


def combine_kernel(parts_ref, cols_ref, phase_ref, dil_ref, out_ref):
    chip, core, _ = place()
    coef = coefficients(cols_ref[...], phase_ref[...])
    lane8 = lane_iota((8, 128))
    row8 = row_iota((8, 128))
    dilution = jnp.broadcast_to(jnp.concatenate([dil_ref[...], dil_ref[...]], axis=1), (8, 128))
    spin_of = lane_xor(dilution, chip & 15, range(4))
    noise_lane = lane8 >= 64
    fields = []
    total = parts_ref[0:40, :]
    for z in range(1, 8):
        total = total + parts_ref[z * 40 : z * 40 + 40, :]
    for time in range(2):
        own = total[time * ROWS : time * ROWS + ROWS]
        terms = []
        for spin in range(4):
            x = jnp.concatenate([own[spin * 4 : spin * 4 + 4], own[16:20]], axis=0)
            for level in range(3):
                row_bit = (row8 >> level) & 1
                lane_bit = (lane8 >> (level + 4)) & 1
                up = pltpu.roll(pltpu.roll(x, 1 << level, 0), 128 - (16 << level), 1)
                down = pltpu.roll(pltpu.roll(x, 8 - (1 << level), 0), 16 << level, 1)
                x = jnp.where(row_bit == lane_bit, x, jnp.where(row_bit == 1, up, down))
            keep = jnp.logical_or(jnp.logical_not(noise_lane), spin_of == spin)
            terms.append(jnp.where(keep, x, 0.0))
        fields.append(dot_exact(coef, jnp.concatenate(terms, axis=0), ((0,), (0,))))
    both = jnp.concatenate(fields, axis=0)
    mirror = lane_xor(both, chip, range(7))
    cross = dot_exact(both, mirror, ((1,), (1,)))
    columns = []
    for time in range(2):
        real = cross[time * 32 : time * 32 + 16]
        imag = cross[time * 32 + 16 : time * 32 + 32]
        for at in (0, 32):
            columns.append(real[:, at : at + 16] - imag[:, at + 16 : at + 32])
            columns.append(real[:, at + 16 : at + 32] + imag[:, at : at + 16])
    trace_rows = jnp.concatenate(columns, axis=1)
    ordered = lane_xor(both, chip & 112, range(4, 7))
    ordered = jnp.where(core == 0, ordered, pltpu.roll(ordered, 120, 1))
    lane = lane_iota((16, 128))
    for pair in range(8):
        rows = jnp.zeros((16, 128), jnp.float32)
        for k in range(4):
            moved = pltpu.roll(ordered[k * 16 : k * 16 + 16], (8 * k - 16 * pair) % 128, 1)
            rows = jnp.where((lane >> 3) == k, moved, rows)
        out_ref[pl.ds(pair * 32, 16, stride=2), :] = trace_rows
        out_ref[pl.ds(pair * 32 + 1, 16, stride=2), :] = rows


def finish_kernel(pairs_ref, got_ref, fields_ref, traces_ref):
    _, _, block = place()
    row = row_iota((32, 128))
    pieces = []
    total = None
    for high in range(16):
        x_high, y_high, x_low, y_low = ((high >> k) & 1 for k in (3, 2, 1, 0))
        at = (x_high * 4 + x_low * 2 + y_low) * 32 + y_high * 2
        piece = got_ref[pl.ds(at, 8, stride=4), :]
        total = piece if total is None else total + piece
        pieces.append(got_ref[pl.ds(at + 1, 8, stride=4), :])
    sums = jnp.sum(total, axis=0, keepdims=True)
    x = jnp.transpose(jnp.concatenate(pieces, axis=0))[0:32, :]
    x = lane_xor(x, block * 8, range(3, 7))
    for bit in range(3):
        x = jnp.where(((row >> bit) & 1) != 0, lane_swap(x, 1 << bit), x)
    for time in range(2):
        for part in range(2):
            at = (time * 2 + part) * 8
            fields_ref[0, time, part] = x[at : at + 8]
    for pair in range(4):
        first = jnp.where(pairs_ref[0, pair] == 0, sums[:, 0:64], sums[:, 64:128])
        picked = jnp.where(pairs_ref[1, pair] == 0, first[:, 0:32], first[:, 32:64]) / 128.0
        traces_ref[pair, 0, 0:1, :] = picked[:, 0:16]
        traces_ref[pair, 0, 1:2, :] = picked[:, 16:32]


def coefficients(cols, phase):
    real = jnp.where(phase == 0, 1.0, jnp.where(phase == 2, -1.0, 0.0))
    imag = jnp.where(phase == 1, 1.0, jnp.where(phase == 3, -1.0, 0.0))
    blocks = []
    for spin in range(4):
        here = jnp.where(cols == spin, 1.0, 0.0)
        blocks.append(jnp.concatenate([here * real, here * imag], axis=1))
        blocks.append(jnp.concatenate([-here * imag, here * real], axis=1))
    return jnp.concatenate(blocks, axis=0)


def in_vmem(x):
    return pltpu.with_memory_space_constraint(x, VMEM)


VMEM_SPEC = pl.BlockSpec(memory_space=VMEM)
HBM_SPEC = pl.BlockSpec(memory_space=pltpu.MemorySpace.HBM)
SMEM_SPEC = pl.BlockSpec(memory_space=pltpu.MemorySpace.SMEM)


def call(kernel, name, out_shape, *operands, specs=None):
    return pl.pallas_call(
        kernel,
        in_specs=specs or [VMEM_SPEC] * len(operands),
        out_specs=jax.tree.map(lambda _: VMEM_SPEC, out_shape),
        out_shape=out_shape,
        compiler_params=pltpu.CompilerParams(vmem_limit_bytes=8 << 20),
        name=name,
    )(*operands)


def local(left_modes, right_modes, gamma_cols, gamma_phase, dilution, time_pairs):
    left = jnp.transpose(left_modes, (0, 1, 2, 4, 3, 5))
    right = jnp.transpose(right_modes, (0, 1, 2, 4, 3, 5))
    dil = dilution.reshape(1, 64)

    partial = products(left, right, dil).reshape(16, 160, 128)
    parts = lax.all_to_all(partial, AXES, 0, 0, axis_index_groups=PLANES, tiled=True)
    plane = call(sum_planes_kernel, "sum_planes", pltpu.VMEM((320, 128), jnp.float32), in_vmem(parts.reshape(2560, 128)))
    parts = lax.all_to_all(plane.reshape(16, 1, 2560), AXES, 0, 0, axis_index_groups=COLUMNS, tiled=True)
    rows = call(
        combine_kernel,
        "combine",
        pltpu.VMEM((256, 128), jnp.float32),
        in_vmem(parts.reshape(320, 128)),
        in_vmem(gamma_cols.T),
        in_vmem(gamma_phase.T),
        in_vmem(dil),
    )
    got = lax.all_to_all(rows.reshape(128, 2, 128), AXES, 0, 0, axis_index_groups=SAME_CORE, tiled=True)
    fields, traces = pl.pallas_call(
        finish_kernel,
        in_specs=[SMEM_SPEC, VMEM_SPEC],
        out_specs=[VMEM_SPEC, VMEM_SPEC],
        out_shape=[
            jax.ShapeDtypeStruct((1, 2, 2, 8, 128), jnp.float32),
            jax.ShapeDtypeStruct((4, 1, 2, 16), jnp.float32),
        ],
        name="finish",
    )(time_pairs.T, in_vmem(got.reshape(256, 128)))
    return (fields, jnp.swapaxes(traces, 2, 3))


def solution(mesh):
    return jax.shard_map(
        local,
        mesh=mesh,
        in_specs=(
            P(None, None, None, None, None, AXES),
            P(None, None, None, None, None, AXES),
            P(),
            P(),
            P(),
            P(),
        ),
        out_specs=(P("gz", None, None, ("gx", "gy"), None), P(None, "gz", None, None)),
        check_vma=False,
    )
```

```python
import jax
import jax.numpy as jnp
from jax import lax
from jax.experimental import pallas as pl
from jax.experimental.pallas import tpu as pltpu
from jax.sharding import PartitionSpec as P

AXES = ("gx", "gy", "gz")
EXACT = lax.Precision.HIGHEST
CHIPS = 128
ROWS = 20
VMEM = pltpu.MemorySpace.VMEM


def flat_index(chip, core):
    bit = [(chip >> k) & 1 for k in range(7)]
    return bit[6] * 128 + bit[4] * 64 + bit[3] * 32 + core * 16 + (chip % 8) * 2 + bit[5]


PLANES = [[flat_index(plane * 8 + z, core) for plane in range(16)] for z in range(8) for core in range(2)]
COLUMNS = [[flat_index(plane * 8 + z, core) for z in range(8) for core in range(2)] for plane in range(16)]
PARTNER = [(flat_index(chip, core), flat_index(chip, 1 - core)) for chip in range(CHIPS) for core in range(2)]
SAME_CORE = [sorted(flat_index(chip, core) for chip in range(CHIPS)) for core in range(2)]


def lane_iota(shape):
    return lax.broadcasted_iota(jnp.int32, shape, len(shape) - 1)


def row_iota(shape):
    return lax.broadcasted_iota(jnp.int32, shape, len(shape) - 2)


def lane_swap(x, step):
    odd = (lane_iota(x.shape) & step) != 0
    return jnp.where(odd, pltpu.roll(x, step, 1), pltpu.roll(x, 128 - step, 1))


def lane_xor(x, amount, bits):
    for bit in bits:
        flip = ((amount >> bit) & 1) != 0
        x = jnp.where(flip, lane_swap(x, 1 << bit), x)
    return x


def place():
    gx, gy, gz = (lax.axis_index(name) for name in AXES)
    chip = (gx >> 1) * 64 + (gz & 1) * 32 + (gx & 1) * 16 + (gy >> 1) * 8 + (gz >> 1)
    return chip, gy & 1, gx * 4 + gy


def fill_rows(right_ref, dil_ref, rows_ref):
    dilution = jnp.broadcast_to(jnp.concatenate([dil_ref[...], dil_ref[...]], axis=1), (128, 128))
    spin_of = jnp.transpose(dilution)[0:64, :]
    pick = []
    for spin in range(4):
        one = jnp.where(spin_of == spin, 1.0, 0.0).astype(jnp.bfloat16)
        pick.append(jnp.concatenate([one] * 4, axis=1))
    for part in range(2):
        for colour in range(3):
            at = (part * 3 + colour) * 512
            noise = None
            for spin in range(4):
                rows_ref[spin * 64 : spin * 64 + 64, at : at + 512] = right_ref[spin, part, colour, 0:64, :]
                term = right_ref[spin, part, colour, 64:128, :] * pick[spin]
                noise = term if noise is None else noise + term
            rows_ref[256:320, at : at + 512] = noise


def add_tile(step, left_ref, rows_ref, out_ref):
    cols = []
    for part in range(2):
        for colour in range(3):
            pieces = []
            for tile in range(2):
                lines = slice(step * 32 + tile * 16, step * 32 + tile * 16 + 16)
                for spin in range(4):
                    pieces.append(left_ref[spin, part, colour, lines, :])
                for spin in range(4):
                    other = left_ref[spin, 1 - part, colour, lines, :]
                    pieces.append(-other if part == 0 else other)
            cols.append(jnp.concatenate(pieces, axis=0))
    prod = lax.dot_general(
        rows_ref[...],
        jnp.concatenate(cols, axis=1),
        (((1,), (1,)), ((), ())),
        preferred_element_type=jnp.float32,
    )
    low_i = lane_iota((8, 128)) & 15
    within = row_iota((8, 128)) ^ (low_i & 7)
    upper = low_i >= 8
    for tile in range(2):
        i_high = step * 2 + tile
        for block in range(20):
            first = prod[block * 16 : block * 16 + 8, tile * 128 : tile * 128 + 128]
            second = prod[block * 16 + 8 : block * 16 + 16, tile * 128 : tile * 128 + 128]
            j_high = block % 4 if block < 16 else block - 12
            start = (i_high ^ j_high) * (16 * ROWS) + block
            low_half = jnp.take_along_axis(jnp.where(upper, second, first), within, axis=0)
            high_half = jnp.take_along_axis(jnp.where(upper, first, second), within, axis=0)
            out_ref[pl.ds(start, 8, stride=ROWS), :] = low_half
            out_ref[pl.ds(start + 8 * ROWS, 8, stride=ROWS), :] = high_half


def away_kernel(
    left_ref, right_ref, dil_ref, out_ref, next_left_ref, next_right_ref, next_dil_ref, rows_ref, left_buf, right_buf, sems
):
    _, core, _ = place()
    copies = [pltpu.make_async_copy(dil_ref, next_dil_ref, sems.at[0])]
    for spin in range(4):
        for part in range(2):
            at = (spin, part)
            sem = sems.at[1 + spin * 2 + part]
            copies.append(pltpu.make_async_copy(right_ref.at[(1 - core,) + at], right_buf.at[at], sem))
    for spin in range(4):
        for part in range(2):
            at = (spin, part)
            sem = sems.at[9 + spin * 2 + part]
            copies.append(pltpu.make_async_copy(left_ref.at[(1 - core,) + at], left_buf.at[at], sem))
    next_copies = []
    for which, (source, target) in enumerate(((right_ref, next_right_ref), (left_ref, next_left_ref))):
        for spin in range(4):
            for part in range(2):
                at = (spin, part)
                sem = sems.at[17 + which * 8 + spin * 2 + part]
                next_copies.append(pltpu.make_async_copy(source.at[(core,) + at], target.at[at], sem))
    for copy in copies + next_copies:
        copy.start()
    for copy in copies:
        copy.wait()
    fill_rows(right_buf, next_dil_ref, rows_ref)
    for step in range(4):
        add_tile(step, left_buf, rows_ref, out_ref)
    for copy in next_copies:
        copy.wait()


def home_kernel(left_ref, right_ref, dil_ref, out_ref, rows_ref):
    fill_rows(right_ref, dil_ref, rows_ref)
    for step in range(4):
        add_tile(step, left_ref, rows_ref, out_ref)


def products(left, right, dil):
    slot = (4, 2, 3, 128, 512)
    rows = pltpu.VMEM((320, 3072), jnp.bfloat16)
    whole = pltpu.VMEM((CHIPS * ROWS, 128), jnp.float32)
    away, next_left, next_right, next_dil = pl.pallas_call(
        away_kernel,
        in_specs=[HBM_SPEC] * 3,
        out_specs=[VMEM_SPEC] * 4,
        out_shape=[whole, pltpu.VMEM(slot, jnp.bfloat16), pltpu.VMEM(slot, jnp.bfloat16), pltpu.VMEM((1, 64), jnp.int32)],
        scratch_shapes=[
            rows,
            pltpu.VMEM(slot, jnp.bfloat16),
            pltpu.VMEM(slot, jnp.bfloat16),
            pltpu.SemaphoreType.DMA((33,)),
        ],
        compiler_params=pltpu.CompilerParams(vmem_limit_bytes=16 << 20),
        name="away",
    )(*(pltpu.with_memory_space_constraint(x, pltpu.MemorySpace.HBM) for x in (left, right, dil)))
    arrived = lax.ppermute(away, AXES, PARTNER)
    home = pl.pallas_call(
        home_kernel,
        in_specs=[VMEM_SPEC] * 3,
        out_specs=VMEM_SPEC,
        out_shape=whole,
        scratch_shapes=[rows],
        compiler_params=pltpu.CompilerParams(vmem_limit_bytes=12 << 20),
        name="home",
    )(in_vmem(next_left), in_vmem(next_right), in_vmem(next_dil))
    return call(add_kernel, "add", whole, in_vmem(home), in_vmem(arrived)), next_dil


def add_kernel(a_ref, b_ref, out_ref):
    out_ref[...] = a_ref[...] + b_ref[...]


def sum_planes_kernel(parts_ref, out_ref):
    total = parts_ref[0:160, :]
    for k in range(1, 16):
        total = total + parts_ref[k * 160 : k * 160 + 160, :]
    for z in range(8):
        mine = total[z * ROWS : z * ROWS + ROWS]
        out_ref[z * 40 : z * 40 + 40, :] = jnp.concatenate([mine, mine], axis=0)


def dot_exact(a, b, dims):
    return lax.dot_general(a, b, (dims, ((), ())), precision=EXACT, preferred_element_type=jnp.float32)


def combine_kernel(parts_ref, cols_ref, phase_ref, dil_ref, out_ref):
    chip, core, _ = place()
    coef = coefficients(cols_ref[...], phase_ref[...])
    lane8 = lane_iota((8, 128))
    row8 = row_iota((8, 128))
    dilution = jnp.broadcast_to(jnp.concatenate([dil_ref[...], dil_ref[...]], axis=1), (8, 128))
    spin_of = lane_xor(dilution, chip & 15, range(4))
    noise_lane = lane8 >= 64
    fields = []
    total = parts_ref[0:40, :]
    for z in range(1, 8):
        total = total + parts_ref[z * 40 : z * 40 + 40, :]
    for time in range(2):
        own = total[time * ROWS : time * ROWS + ROWS]
        terms = []
        for spin in range(4):
            x = jnp.concatenate([own[spin * 4 : spin * 4 + 4], own[16:20]], axis=0)
            for level in range(3):
                row_bit = (row8 >> level) & 1
                lane_bit = (lane8 >> (level + 4)) & 1
                up = pltpu.roll(pltpu.roll(x, 1 << level, 0), 128 - (16 << level), 1)
                down = pltpu.roll(pltpu.roll(x, 8 - (1 << level), 0), 16 << level, 1)
                x = jnp.where(row_bit == lane_bit, x, jnp.where(row_bit == 1, up, down))
            keep = jnp.logical_or(jnp.logical_not(noise_lane), spin_of == spin)
            terms.append(jnp.where(keep, x, 0.0))
        fields.append(dot_exact(coef, jnp.concatenate(terms, axis=0), ((0,), (0,))))
    both = jnp.concatenate(fields, axis=0)
    mirror = lane_xor(both, chip, range(7))
    cross = dot_exact(both, mirror, ((1,), (1,)))
    columns = []
    for time in range(2):
        real = cross[time * 32 : time * 32 + 16]
        imag = cross[time * 32 + 16 : time * 32 + 32]
        for at in (0, 32):
            columns.append(real[:, at : at + 16] - imag[:, at + 16 : at + 32])
            columns.append(real[:, at + 16 : at + 32] + imag[:, at : at + 16])
    trace_rows = jnp.concatenate(columns, axis=1)
    ordered = lane_xor(both, chip & 112, range(4, 7))
    ordered = jnp.where(core == 0, ordered, pltpu.roll(ordered, 120, 1))
    lane = lane_iota((16, 128))
    for pair in range(8):
        rows = jnp.zeros((16, 128), jnp.float32)
        for k in range(4):
            moved = pltpu.roll(ordered[k * 16 : k * 16 + 16], (8 * k - 16 * pair) % 128, 1)
            rows = jnp.where((lane >> 3) == k, moved, rows)
        out_ref[pl.ds(pair * 32, 16, stride=2), :] = trace_rows
        out_ref[pl.ds(pair * 32 + 1, 16, stride=2), :] = rows


def finish_kernel(pairs_ref, got_ref, fields_ref, traces_ref):
    _, _, block = place()
    row = row_iota((32, 128))
    pieces = []
    total = None
    for high in range(16):
        x_high, y_high, x_low, y_low = ((high >> k) & 1 for k in (3, 2, 1, 0))
        at = (x_high * 4 + x_low * 2 + y_low) * 32 + y_high * 2
        piece = got_ref[pl.ds(at, 8, stride=4), :]
        total = piece if total is None else total + piece
        pieces.append(got_ref[pl.ds(at + 1, 8, stride=4), :])
    sums = jnp.sum(total, axis=0, keepdims=True)
    x = jnp.transpose(jnp.concatenate(pieces, axis=0))[0:32, :]
    x = lane_xor(x, block * 8, range(3, 7))
    for bit in range(3):
        x = jnp.where(((row >> bit) & 1) != 0, lane_swap(x, 1 << bit), x)
    for time in range(2):
        for part in range(2):
            at = (time * 2 + part) * 8
            fields_ref[0, time, part] = x[at : at + 8]
    for pair in range(4):
        first = jnp.where(pairs_ref[0, pair] == 0, sums[:, 0:64], sums[:, 64:128])
        picked = jnp.where(pairs_ref[1, pair] == 0, first[:, 0:32], first[:, 32:64]) / 128.0
        traces_ref[pair, 0, 0:1, :] = picked[:, 0:16]
        traces_ref[pair, 0, 1:2, :] = picked[:, 16:32]


def coefficients(cols, phase):
    real = jnp.where(phase == 0, 1.0, jnp.where(phase == 2, -1.0, 0.0))
    imag = jnp.where(phase == 1, 1.0, jnp.where(phase == 3, -1.0, 0.0))
    blocks = []
    for spin in range(4):
        here = jnp.where(cols == spin, 1.0, 0.0)
        blocks.append(jnp.concatenate([here * real, here * imag], axis=1))
        blocks.append(jnp.concatenate([-here * imag, here * real], axis=1))
    return jnp.concatenate(blocks, axis=0)


def in_vmem(x):
    return pltpu.with_memory_space_constraint(x, VMEM)


VMEM_SPEC = pl.BlockSpec(memory_space=VMEM)
HBM_SPEC = pl.BlockSpec(memory_space=pltpu.MemorySpace.HBM)
SMEM_SPEC = pl.BlockSpec(memory_space=pltpu.MemorySpace.SMEM)


def call(kernel, name, out_shape, *operands, specs=None):
    return pl.pallas_call(
        kernel,
        in_specs=specs or [VMEM_SPEC] * len(operands),
        out_specs=jax.tree.map(lambda _: VMEM_SPEC, out_shape),
        out_shape=out_shape,
        compiler_params=pltpu.CompilerParams(vmem_limit_bytes=8 << 20),
        name=name,
    )(*operands)


def local(left_modes, right_modes, gamma_cols, gamma_phase, dilution, time_pairs):
    left = jnp.transpose(left_modes, (0, 1, 2, 4, 3, 5))
    right = jnp.transpose(right_modes, (0, 1, 2, 4, 3, 5))
    dil = dilution.reshape(1, 64)

    partial, dil = products(left, right, dil)
    partial = partial.reshape(16, 160, 128)
    parts = lax.all_to_all(partial, AXES, 0, 0, axis_index_groups=PLANES, tiled=True)
    plane = call(sum_planes_kernel, "sum_planes", pltpu.VMEM((320, 128), jnp.float32), in_vmem(parts.reshape(2560, 128)))
    parts = lax.all_to_all(plane.reshape(16, 1, 2560), AXES, 0, 0, axis_index_groups=COLUMNS, tiled=True)
    rows = call(
        combine_kernel,
        "combine",
        pltpu.VMEM((256, 128), jnp.float32),
        in_vmem(parts.reshape(320, 128)),
        in_vmem(gamma_cols.T),
        in_vmem(gamma_phase.T),
        in_vmem(dil),
    )
    got = lax.all_to_all(rows.reshape(128, 2, 128), AXES, 0, 0, axis_index_groups=SAME_CORE, tiled=True)
    fields, traces = pl.pallas_call(
        finish_kernel,
        in_specs=[SMEM_SPEC, VMEM_SPEC],
        out_specs=[VMEM_SPEC, VMEM_SPEC],
        out_shape=[
            jax.ShapeDtypeStruct((1, 2, 2, 8, 128), jnp.float32),
            jax.ShapeDtypeStruct((4, 1, 2, 16), jnp.float32),
        ],
        name="finish",
    )(time_pairs.T, in_vmem(got.reshape(256, 128)))
    return (fields, jnp.swapaxes(traces, 2, 3))


def solution(mesh):
    return jax.shard_map(
        local,
        mesh=mesh,
        in_specs=(
            P(None, None, None, None, None, AXES),
            P(None, None, None, None, None, AXES),
            P(),
            P(),
            P(),
            P(),
        ),
        out_specs=(P("gz", None, None, ("gx", "gy"), None), P(None, "gz", None, None)),
        check_vma=False,
    )
```

```python
import jax
import jax.numpy as jnp
from jax import lax
from jax.experimental import pallas as pl
from jax.experimental.pallas import tpu as pltpu
from jax.sharding import PartitionSpec as P

AXES = ("gx", "gy", "gz")
EXACT = lax.Precision.HIGHEST
CHIPS = 128
ROWS = 20
VMEM = pltpu.MemorySpace.VMEM


def flat_index(chip, core):
    bit = [(chip >> k) & 1 for k in range(7)]
    return bit[6] * 128 + bit[4] * 64 + bit[3] * 32 + core * 16 + (chip % 8) * 2 + bit[5]


PLANES = [[flat_index(plane * 8 + z, core) for plane in range(16)] for z in range(8) for core in range(2)]
COLUMNS = [[flat_index(plane * 8 + z, core) for z in range(8) for core in range(2)] for plane in range(16)]
PARTNER = [(flat_index(chip, core), flat_index(chip, 1 - core)) for chip in range(CHIPS) for core in range(2)]
SAME_CORE = [sorted(flat_index(chip, core) for chip in range(CHIPS)) for core in range(2)]


def lane_iota(shape):
    return lax.broadcasted_iota(jnp.int32, shape, len(shape) - 1)


def row_iota(shape):
    return lax.broadcasted_iota(jnp.int32, shape, len(shape) - 2)


def lane_swap(x, step):
    odd = (lane_iota(x.shape) & step) != 0
    return jnp.where(odd, pltpu.roll(x, step, 1), pltpu.roll(x, 128 - step, 1))


def lane_xor(x, amount, bits):
    for bit in bits:
        flip = ((amount >> bit) & 1) != 0
        x = jnp.where(flip, lane_swap(x, 1 << bit), x)
    return x


def place():
    gx, gy, gz = (lax.axis_index(name) for name in AXES)
    chip = (gx >> 1) * 64 + (gz & 1) * 32 + (gx & 1) * 16 + (gy >> 1) * 8 + (gz >> 1)
    return chip, gy & 1, gx * 4 + gy


def fill_rows(right_ref, dil_ref, rows_ref):
    dilution = jnp.broadcast_to(jnp.concatenate([dil_ref[...], dil_ref[...]], axis=1), (128, 128))
    spin_of = jnp.transpose(dilution)[0:64, :]
    pick = []
    for spin in range(4):
        one = jnp.where(spin_of == spin, 1.0, 0.0).astype(jnp.bfloat16)
        pick.append(jnp.concatenate([one] * 4, axis=1))
    for part in range(2):
        for colour in range(3):
            at = (part * 3 + colour) * 512
            noise = None
            for spin in range(4):
                rows_ref[spin * 64 : spin * 64 + 64, at : at + 512] = right_ref[spin, part, colour, 0:64, :]
                term = right_ref[spin, part, colour, 64:128, :] * pick[spin]
                noise = term if noise is None else noise + term
            rows_ref[256:320, at : at + 512] = noise


def add_tile(step, left_ref, rows_ref, out_ref):
    cols = []
    for part in range(2):
        for colour in range(3):
            pieces = []
            for tile in range(2):
                lines = slice(step * 32 + tile * 16, step * 32 + tile * 16 + 16)
                for spin in range(4):
                    pieces.append(left_ref[spin, part, colour, lines, :])
                for spin in range(4):
                    other = left_ref[spin, 1 - part, colour, lines, :]
                    pieces.append(-other if part == 0 else other)
            cols.append(jnp.concatenate(pieces, axis=0))
    prod = lax.dot_general(
        rows_ref[...],
        jnp.concatenate(cols, axis=1),
        (((1,), (1,)), ((), ())),
        preferred_element_type=jnp.float32,
    )
    low_i = lane_iota((8, 128)) & 15
    within = row_iota((8, 128)) ^ (low_i & 7)
    upper = low_i >= 8
    for tile in range(2):
        i_high = step * 2 + tile
        for block in range(20):
            first = prod[block * 16 : block * 16 + 8, tile * 128 : tile * 128 + 128]
            second = prod[block * 16 + 8 : block * 16 + 16, tile * 128 : tile * 128 + 128]
            j_high = block % 4 if block < 16 else block - 12
            start = (i_high ^ j_high) * (16 * ROWS) + block
            low_half = jnp.take_along_axis(jnp.where(upper, second, first), within, axis=0)
            high_half = jnp.take_along_axis(jnp.where(upper, first, second), within, axis=0)
            out_ref[pl.ds(start, 8, stride=ROWS), :] = low_half
            out_ref[pl.ds(start + 8 * ROWS, 8, stride=ROWS), :] = high_half


def away_kernel(
    left_ref, right_ref, dil_ref, out_ref, next_left_ref, next_right_ref, next_dil_ref, rows_ref, left_buf, right_buf, sems
):
    _, core, _ = place()
    copies = [pltpu.make_async_copy(dil_ref, next_dil_ref, sems.at[0])]
    for spin in range(4):
        for part in range(2):
            at = (spin, part)
            sem = sems.at[1 + spin * 2 + part]
            copies.append(pltpu.make_async_copy(right_ref.at[(1 - core,) + at], right_buf.at[at], sem))
    for spin in range(4):
        for part in range(2):
            at = (spin, part)
            sem = sems.at[9 + spin * 2 + part]
            copies.append(pltpu.make_async_copy(left_ref.at[(1 - core,) + at], left_buf.at[at], sem))
    next_copies = []
    for which, (source, target) in enumerate(((right_ref, next_right_ref), (left_ref, next_left_ref))):
        for spin in range(4):
            for part in range(2):
                at = (spin, part)
                sem = sems.at[17 + which * 8 + spin * 2 + part]
                next_copies.append(pltpu.make_async_copy(source.at[(core,) + at], target.at[at], sem))
    for copy in copies + next_copies:
        copy.start()
    for copy in copies:
        copy.wait()
    fill_rows(right_buf, next_dil_ref, rows_ref)
    for step in range(4):
        add_tile(step, left_buf, rows_ref, out_ref)
    for copy in next_copies:
        copy.wait()


def home_kernel(left_ref, right_ref, dil_ref, out_ref, rows_ref):
    fill_rows(right_ref, dil_ref, rows_ref)
    for step in range(4):
        add_tile(step, left_ref, rows_ref, out_ref)


def products(left, right, dil):
    slot = (4, 2, 3, 128, 512)
    rows = pltpu.VMEM((320, 3072), jnp.bfloat16)
    whole = pltpu.VMEM((CHIPS * ROWS, 128), jnp.float32)
    away, next_left, next_right, next_dil = pl.pallas_call(
        away_kernel,
        in_specs=[HBM_SPEC] * 3,
        out_specs=[VMEM_SPEC] * 4,
        out_shape=[whole, pltpu.VMEM(slot, jnp.bfloat16), pltpu.VMEM(slot, jnp.bfloat16), pltpu.VMEM((1, 64), jnp.int32)],
        scratch_shapes=[
            rows,
            pltpu.VMEM(slot, jnp.bfloat16),
            pltpu.VMEM(slot, jnp.bfloat16),
            pltpu.SemaphoreType.DMA((33,)),
        ],
        compiler_params=pltpu.CompilerParams(vmem_limit_bytes=16 << 20),
        name="away",
    )(*(pltpu.with_memory_space_constraint(x, pltpu.MemorySpace.HBM) for x in (left, right, dil)))
    arrived = lax.ppermute(away, AXES, PARTNER)
    home = pl.pallas_call(
        home_kernel,
        in_specs=[VMEM_SPEC] * 3,
        out_specs=VMEM_SPEC,
        out_shape=whole,
        scratch_shapes=[rows],
        compiler_params=pltpu.CompilerParams(vmem_limit_bytes=12 << 20),
        name="home",
    )(in_vmem(next_left), in_vmem(next_right), in_vmem(next_dil))
    return call(add_kernel, "add", whole, in_vmem(home), in_vmem(arrived)), next_dil


def add_kernel(a_ref, b_ref, out_ref):
    out_ref[...] = a_ref[...] + b_ref[...]


def sum_planes_kernel(parts_ref, out_ref):
    total = parts_ref[0:160, :]
    for k in range(1, 16):
        total = total + parts_ref[k * 160 : k * 160 + 160, :]
    for z in range(8):
        mine = total[z * ROWS : z * ROWS + ROWS]
        out_ref[z * 40 : z * 40 + 40, :] = jnp.concatenate([mine, mine], axis=0)


def dot_exact(a, b, dims):
    return lax.dot_general(a, b, (dims, ((), ())), precision=EXACT, preferred_element_type=jnp.float32)


def combine_kernel(parts_ref, cols_ref, phase_ref, dil_ref, pairs_ref, out_ref):
    chip, core, _ = place()
    coef = coefficients(cols_ref[...], phase_ref[...])
    lane8 = lane_iota((8, 128))
    row8 = row_iota((8, 128))
    dilution = jnp.broadcast_to(jnp.concatenate([dil_ref[...], dil_ref[...]], axis=1), (8, 128))
    spin_of = lane_xor(dilution, chip & 15, range(4))
    noise_lane = lane8 >= 64
    fields = []
    total = parts_ref[0:40, :]
    for z in range(1, 8):
        total = total + parts_ref[z * 40 : z * 40 + 40, :]
    for time in range(2):
        own = total[time * ROWS : time * ROWS + ROWS]
        terms = []
        for spin in range(4):
            x = jnp.concatenate([own[spin * 4 : spin * 4 + 4], own[16:20]], axis=0)
            for level in range(3):
                row_bit = (row8 >> level) & 1
                lane_bit = (lane8 >> (level + 4)) & 1
                up = pltpu.roll(pltpu.roll(x, 1 << level, 0), 128 - (16 << level), 1)
                down = pltpu.roll(pltpu.roll(x, 8 - (1 << level), 0), 16 << level, 1)
                x = jnp.where(row_bit == lane_bit, x, jnp.where(row_bit == 1, up, down))
            keep = jnp.logical_or(jnp.logical_not(noise_lane), spin_of == spin)
            terms.append(jnp.where(keep, x, 0.0))
        fields.append(dot_exact(coef, jnp.concatenate(terms, axis=0), ((0,), (0,))))
    both = jnp.concatenate(fields, axis=0)
    mirror = lane_xor(both, chip, range(7))
    cross = dot_exact(both, mirror, ((1,), (1,)))
    crossed = []
    for time in range(2):
        real = cross[time * 32 : time * 32 + 16]
        imag = cross[time * 32 + 16 : time * 32 + 32]
        for at in (0, 32):
            real_part = real[:, at : at + 16] - imag[:, at + 16 : at + 32]
            imag_part = real[:, at + 16 : at + 32] + imag[:, at : at + 16]
            crossed.append(jnp.concatenate([real_part, imag_part], axis=1))
    columns = []
    for pair in range(4):
        first = jnp.broadcast_to(pairs_ref[0:1, pair : pair + 1], (16, 32)) == 0
        second = jnp.broadcast_to(pairs_ref[1:2, pair : pair + 1], (16, 32)) == 0
        columns.append(
            jnp.where(first, jnp.where(second, crossed[0], crossed[1]), jnp.where(second, crossed[2], crossed[3]))
        )
    trace_rows = jnp.concatenate(columns, axis=1)
    ordered = lane_xor(both, chip & 112, range(4, 7))
    ordered = jnp.where(core == 0, ordered, pltpu.roll(ordered, 120, 1))
    lane = lane_iota((16, 128))
    for pair in range(8):
        rows = jnp.zeros((16, 128), jnp.float32)
        for k in range(4):
            moved = pltpu.roll(ordered[k * 16 : k * 16 + 16], (8 * k - 16 * pair) % 128, 1)
            rows = jnp.where((lane >> 3) == k, moved, rows)
        out_ref[pl.ds(pair * 32, 16, stride=2), :] = trace_rows
        out_ref[pl.ds(pair * 32 + 1, 16, stride=2), :] = rows


def finish_kernel(got_ref, fields_ref, traces_ref):
    _, _, block = place()
    row = row_iota((32, 128))
    pieces = []
    total = None
    for high in range(16):
        x_high, y_high, x_low, y_low = ((high >> k) & 1 for k in (3, 2, 1, 0))
        at = (x_high * 4 + x_low * 2 + y_low) * 32 + y_high * 2
        piece = got_ref[pl.ds(at, 8, stride=4), :]
        total = piece if total is None else total + piece
        pieces.append(got_ref[pl.ds(at + 1, 8, stride=4), :])
    sums = jnp.sum(total, axis=0, keepdims=True)
    x = jnp.transpose(jnp.concatenate(pieces, axis=0))[0:32, :]
    x = lane_xor(x, block * 8, range(3, 7))
    for bit in range(3):
        x = jnp.where(((row >> bit) & 1) != 0, lane_swap(x, 1 << bit), x)
    for time in range(2):
        for part in range(2):
            at = (time * 2 + part) * 8
            fields_ref[0, time, part] = x[at : at + 8]
    sums = sums / 128.0
    for pair in range(4):
        traces_ref[pair, 0, 0:1, :] = sums[:, pair * 32 : pair * 32 + 16]
        traces_ref[pair, 0, 1:2, :] = sums[:, pair * 32 + 16 : pair * 32 + 32]


def coefficients(cols, phase):
    real = jnp.where(phase == 0, 1.0, jnp.where(phase == 2, -1.0, 0.0))
    imag = jnp.where(phase == 1, 1.0, jnp.where(phase == 3, -1.0, 0.0))
    blocks = []
    for spin in range(4):
        here = jnp.where(cols == spin, 1.0, 0.0)
        blocks.append(jnp.concatenate([here * real, here * imag], axis=1))
        blocks.append(jnp.concatenate([-here * imag, here * real], axis=1))
    return jnp.concatenate(blocks, axis=0)


def in_vmem(x):
    return pltpu.with_memory_space_constraint(x, VMEM)


VMEM_SPEC = pl.BlockSpec(memory_space=VMEM)
HBM_SPEC = pl.BlockSpec(memory_space=pltpu.MemorySpace.HBM)


def call(kernel, name, out_shape, *operands, specs=None):
    return pl.pallas_call(
        kernel,
        in_specs=specs or [VMEM_SPEC] * len(operands),
        out_specs=jax.tree.map(lambda _: VMEM_SPEC, out_shape),
        out_shape=out_shape,
        compiler_params=pltpu.CompilerParams(vmem_limit_bytes=8 << 20),
        name=name,
    )(*operands)


def local(left_modes, right_modes, gamma_cols, gamma_phase, dilution, time_pairs):
    left = jnp.transpose(left_modes, (0, 1, 2, 4, 3, 5))
    right = jnp.transpose(right_modes, (0, 1, 2, 4, 3, 5))
    dil = dilution.reshape(1, 64)

    partial, dil = products(left, right, dil)
    partial = partial.reshape(16, 160, 128)
    parts = lax.all_to_all(partial, AXES, 0, 0, axis_index_groups=PLANES, tiled=True)
    plane = call(sum_planes_kernel, "sum_planes", pltpu.VMEM((320, 128), jnp.float32), in_vmem(parts.reshape(2560, 128)))
    parts = lax.all_to_all(plane.reshape(16, 1, 2560), AXES, 0, 0, axis_index_groups=COLUMNS, tiled=True)
    rows = call(
        combine_kernel,
        "combine",
        pltpu.VMEM((256, 128), jnp.float32),
        in_vmem(parts.reshape(320, 128)),
        in_vmem(gamma_cols.T),
        in_vmem(gamma_phase.T),
        in_vmem(dil),
        in_vmem(time_pairs.T),
    )
    got = lax.all_to_all(rows.reshape(128, 2, 128), AXES, 0, 0, axis_index_groups=SAME_CORE, tiled=True)
    fields, traces = pl.pallas_call(
        finish_kernel,
        in_specs=[VMEM_SPEC],
        out_specs=[VMEM_SPEC, VMEM_SPEC],
        out_shape=[
            jax.ShapeDtypeStruct((1, 2, 2, 8, 128), jnp.float32),
            jax.ShapeDtypeStruct((4, 1, 2, 16), jnp.float32),
        ],
        name="finish",
    )(in_vmem(got.reshape(256, 128)))
    return (fields, jnp.swapaxes(traces, 2, 3))


def solution(mesh):
    return jax.shard_map(
        local,
        mesh=mesh,
        in_specs=(
            P(None, None, None, None, None, AXES),
            P(None, None, None, None, None, AXES),
            P(),
            P(),
            P(),
            P(),
        ),
        out_specs=(P("gz", None, None, ("gx", "gy"), None), P(None, "gz", None, None)),
        check_vma=False,
    )
```

```python
import jax
import jax.numpy as jnp
from jax import lax
from jax.experimental import pallas as pl
from jax.experimental.pallas import tpu as pltpu
from jax.sharding import PartitionSpec as P

AXES = ("gx", "gy", "gz")
EXACT = lax.Precision.HIGHEST
CHIPS = 128
ROWS = 20
VMEM = pltpu.MemorySpace.VMEM


def flat_index(chip, core):
    bit = [(chip >> k) & 1 for k in range(7)]
    return bit[6] * 128 + bit[4] * 64 + bit[3] * 32 + core * 16 + (chip % 8) * 2 + bit[5]


PLANES = [[flat_index(plane * 8 + z, core) for plane in range(16)] for z in range(8) for core in range(2)]
COLUMNS = [[flat_index(plane * 8 + z, core) for core in range(2) for z in range(8)] for plane in range(16)]
PARTNER = [(flat_index(chip, core), flat_index(chip, 1 - core)) for chip in range(CHIPS) for core in range(2)]
SAME_CORE = [sorted(flat_index(chip, core) for chip in range(CHIPS)) for core in range(2)]


def lane_iota(shape):
    return lax.broadcasted_iota(jnp.int32, shape, len(shape) - 1)


def row_iota(shape):
    return lax.broadcasted_iota(jnp.int32, shape, len(shape) - 2)


def place():
    gx, gy, gz = (lax.axis_index(name) for name in AXES)
    chip = (gx >> 1) * 64 + (gz & 1) * 32 + (gx & 1) * 16 + (gy >> 1) * 8 + (gz >> 1)
    return chip, gy & 1, gx * 4 + gy


def fill_rows(right_ref, dil_ref, rows_ref):
    dilution = jnp.broadcast_to(jnp.concatenate([dil_ref[...], dil_ref[...]], axis=1), (128, 128))
    spin_of = jnp.transpose(dilution)[0:64, :]
    pick = []
    for spin in range(4):
        one = jnp.where(spin_of == spin, 1.0, 0.0).astype(jnp.bfloat16)
        pick.append(jnp.concatenate([one] * 4, axis=1))
    for part in range(2):
        for colour in range(3):
            at = (part * 3 + colour) * 512
            noise = None
            for spin in range(4):
                rows_ref[spin * 64 : spin * 64 + 64, at : at + 512] = right_ref[spin, part, colour, 0:64, :]
                term = right_ref[spin, part, colour, 64:128, :] * pick[spin]
                noise = term if noise is None else noise + term
            rows_ref[256:320, at : at + 512] = noise


def add_tile(step, left_ref, rows_ref, out_ref):
    cols = []
    for part in range(2):
        for colour in range(3):
            pieces = []
            for tile in range(2):
                lines = slice(step * 32 + tile * 16, step * 32 + tile * 16 + 16)
                for spin in range(4):
                    pieces.append(left_ref[spin, part, colour, lines, :])
                for spin in range(4):
                    other = left_ref[spin, 1 - part, colour, lines, :]
                    pieces.append(-other if part == 0 else other)
            cols.append(jnp.concatenate(pieces, axis=0))
    prod = lax.dot_general(
        rows_ref[...],
        jnp.concatenate(cols, axis=1),
        (((1,), (1,)), ((), ())),
        preferred_element_type=jnp.float32,
    )
    low_i = lane_iota((8, 128)) & 15
    within = row_iota((8, 128)) ^ (low_i & 7)
    upper = low_i >= 8
    for tile in range(2):
        i_high = step * 2 + tile
        for block in range(20):
            first = prod[block * 16 : block * 16 + 8, tile * 128 : tile * 128 + 128]
            second = prod[block * 16 + 8 : block * 16 + 16, tile * 128 : tile * 128 + 128]
            j_high = block % 4 if block < 16 else block - 12
            start = (i_high ^ j_high) * (16 * ROWS) + block
            low_half = jnp.take_along_axis(jnp.where(upper, second, first), within, axis=0)
            high_half = jnp.take_along_axis(jnp.where(upper, first, second), within, axis=0)
            out_ref[pl.ds(start, 8, stride=ROWS), :] = low_half
            out_ref[pl.ds(start + 8 * ROWS, 8, stride=ROWS), :] = high_half


def away_kernel(
    left_ref, right_ref, dil_ref, cols_ref, phase_ref, out_ref, next_left_ref, next_right_ref, next_dil_ref, coef_ref, spin_ref,
    rows_ref, left_buf, right_buf, cols_buf, phase_buf, sems
):
    chip, core, _ = place()
    small = [
        pltpu.make_async_copy(dil_ref, next_dil_ref, sems.at[0]),
        pltpu.make_async_copy(cols_ref, cols_buf, sems.at[33]),
        pltpu.make_async_copy(phase_ref, phase_buf, sems.at[34]),
    ]
    copies = []
    for spin in range(4):
        for part in range(2):
            at = (spin, part)
            sem = sems.at[1 + spin * 2 + part]
            copies.append(pltpu.make_async_copy(right_ref.at[(1 - core,) + at], right_buf.at[at], sem))
    for spin in range(4):
        for part in range(2):
            at = (spin, part)
            sem = sems.at[9 + spin * 2 + part]
            copies.append(pltpu.make_async_copy(left_ref.at[(1 - core,) + at], left_buf.at[at], sem))
    next_copies = []
    for which, (source, target) in enumerate(((right_ref, next_right_ref), (left_ref, next_left_ref))):
        for spin in range(4):
            for part in range(2):
                at = (spin, part)
                sem = sems.at[17 + which * 8 + spin * 2 + part]
                next_copies.append(pltpu.make_async_copy(source.at[(core,) + at], target.at[at], sem))
    for copy in small + copies + next_copies:
        copy.start()
    for copy in small:
        copy.wait()
    coef_ref[...] = coefficients(cols_buf[...], phase_buf[...])
    dilution = jnp.broadcast_to(jnp.concatenate([next_dil_ref[...], next_dil_ref[...]], axis=1), (8, 128))
    spin_ref[...] = lane_pick(dilution, lane_iota((8, 128)) ^ (chip & 15))
    for copy in copies:
        copy.wait()
    fill_rows(right_buf, next_dil_ref, rows_ref)
    for step in range(4):
        add_tile(step, left_buf, rows_ref, out_ref)
    for copy in next_copies:
        copy.wait()


def home_kernel(left_ref, right_ref, dil_ref, out_ref, rows_ref):
    fill_rows(right_ref, dil_ref, rows_ref)
    for step in range(4):
        add_tile(step, left_ref, rows_ref, out_ref)


def products(left, right, dil, cols, phase):
    slot = (4, 2, 3, 128, 512)
    rows = pltpu.VMEM((320, 3072), jnp.bfloat16)
    whole = pltpu.VMEM((CHIPS * ROWS, 128), jnp.float32)
    away, next_left, next_right, next_dil, coef, spin_of = pl.pallas_call(
        away_kernel,
        in_specs=[HBM_SPEC] * 5,
        out_specs=[VMEM_SPEC] * 6,
        out_shape=[
            whole,
            pltpu.VMEM(slot, jnp.bfloat16),
            pltpu.VMEM(slot, jnp.bfloat16),
            pltpu.VMEM((1, 64), jnp.int32),
            pltpu.VMEM((32, 32), jnp.float32),
            pltpu.VMEM((8, 128), jnp.int32),
        ],
        scratch_shapes=[
            rows,
            pltpu.VMEM(slot, jnp.bfloat16),
            pltpu.VMEM(slot, jnp.bfloat16),
            pltpu.VMEM((4, 16), jnp.int32),
            pltpu.VMEM((4, 16), jnp.int32),
            pltpu.SemaphoreType.DMA((35,)),
        ],
        compiler_params=pltpu.CompilerParams(vmem_limit_bytes=16 << 20),
        name="away",
    )(*(pltpu.with_memory_space_constraint(x, pltpu.MemorySpace.HBM) for x in (left, right, dil, cols, phase)))
    arrived = lax.ppermute(away, AXES, PARTNER)
    home = pl.pallas_call(
        home_kernel,
        in_specs=[VMEM_SPEC] * 3,
        out_specs=VMEM_SPEC,
        out_shape=whole,
        scratch_shapes=[rows],
        compiler_params=pltpu.CompilerParams(vmem_limit_bytes=12 << 20),
        name="home",
    )(in_vmem(next_left), in_vmem(next_right), in_vmem(next_dil))
    return call(add_kernel, "add", whole, in_vmem(home), in_vmem(arrived)), coef, spin_of


def add_kernel(a_ref, b_ref, out_ref):
    out_ref[...] = a_ref[...] + b_ref[...]


def sum_planes_kernel(parts_ref, out_ref):
    total = parts_ref[0:160, :]
    for k in range(1, 16):
        total = total + parts_ref[k * 160 : k * 160 + 160, :]
    for z in range(8):
        mine = total[z * ROWS : z * ROWS + ROWS]
        out_ref[z * ROWS : z * ROWS + ROWS, :] = mine
        out_ref[160 + z * ROWS : 160 + z * ROWS + ROWS, :] = mine


def dot_exact(a, b, dims):
    return lax.dot_general(a, b, (dims, ((), ())), precision=EXACT, preferred_element_type=jnp.float32)


def lane_pick(x, lanes):
    return jnp.take_along_axis(x, lanes, axis=1)


def combine_kernel(parts_ref, coef_ref, spin_ref, pairs_ref, out_ref):
    chip, core, _ = place()
    lane8 = lane_iota((8, 128))
    row8 = row_iota((8, 128))
    block = lane8 >> 4
    turn = ((block + row8) & 7) * 16 + (lane8 & 15)
    fall = (row8 - block) & 7
    back = ((row8 - block) & 7) * 16 + (lane8 & 15)
    spin_of = spin_ref[...]
    fields = []
    for time in range(2):
        total = parts_ref[time * 160 : time * 160 + ROWS, :]
        for z in range(1, 8):
            at = time * 160 + z * ROWS
            total = total + parts_ref[at : at + ROWS, :]
        terms = []
        for spin in range(4):
            x = jnp.concatenate([total[spin * 4 : spin * 4 + 4], total[16:20]], axis=0)
            x = lane_pick(jnp.take_along_axis(lane_pick(x, turn), fall, axis=0), back)
            keep = jnp.logical_or(lane8 < 64, spin_of == spin)
            terms.append(jnp.where(keep, x, 0.0))
        fields.append(dot_exact(coef_ref[...], jnp.concatenate(terms, axis=0), ((0,), (0,))))
    both = jnp.concatenate(fields, axis=0)
    lanes = lane_iota((64, 128))
    mirror = lane_pick(both, lanes ^ chip)
    cross = dot_exact(both, mirror, ((1,), (1,)))
    crossed = []
    for time in range(2):
        real = cross[time * 32 : time * 32 + 16]
        imag = cross[time * 32 + 16 : time * 32 + 32]
        for at in (0, 32):
            real_part = real[:, at : at + 16] - imag[:, at + 16 : at + 32]
            imag_part = real[:, at + 16 : at + 32] + imag[:, at : at + 16]
            crossed.append(jnp.concatenate([real_part, imag_part], axis=1))
    columns = []
    for pair in range(4):
        first = jnp.broadcast_to(pairs_ref[0:1, pair : pair + 1], (16, 32)) == 0
        second = jnp.broadcast_to(pairs_ref[1:2, pair : pair + 1], (16, 32)) == 0
        columns.append(
            jnp.where(first, jnp.where(second, crossed[0], crossed[1]), jnp.where(second, crossed[2], crossed[3]))
        )
    trace_rows = jnp.concatenate(columns, axis=1)
    ordered = lane_pick(both, ((lanes + 8 * core) & 127) ^ (chip & 112))
    lane = lane_iota((16, 128))
    for pair in range(8):
        rows = jnp.zeros((16, 128), jnp.float32)
        for k in range(4):
            moved = pltpu.roll(ordered[k * 16 : k * 16 + 16], (8 * k - 16 * pair) % 128, 1)
            rows = jnp.where((lane >> 3) == k, moved, rows)
        out_ref[pl.ds(pair * 32, 16, stride=2), :] = trace_rows
        out_ref[pl.ds(pair * 32 + 1, 16, stride=2), :] = rows


def finish_kernel(got_ref, fields_ref, traces_ref):
    _, _, block = place()
    row = row_iota((32, 128))
    pieces = []
    total = None
    for high in range(16):
        x_high, y_high, x_low, y_low = ((high >> k) & 1 for k in (3, 2, 1, 0))
        at = (x_high * 4 + x_low * 2 + y_low) * 32 + y_high * 2
        piece = got_ref[pl.ds(at, 8, stride=4), :]
        total = piece if total is None else total + piece
        pieces.append(got_ref[pl.ds(at + 1, 8, stride=4), :])
    sums = jnp.sum(total, axis=0, keepdims=True)
    x = jnp.transpose(jnp.concatenate(pieces, axis=0))[0:32, :]
    x = lane_pick(x, lane_iota((32, 128)) ^ (block * 8 + (row & 7)))
    for time in range(2):
        for part in range(2):
            at = (time * 2 + part) * 8
            fields_ref[0, time, part] = x[at : at + 8]
    sums = sums / 128.0
    for pair in range(4):
        traces_ref[pair, 0, 0:1, :] = sums[:, pair * 32 : pair * 32 + 16]
        traces_ref[pair, 0, 1:2, :] = sums[:, pair * 32 + 16 : pair * 32 + 32]


def coefficients(cols, phase):
    real = jnp.where(phase == 0, 1.0, jnp.where(phase == 2, -1.0, 0.0))
    imag = jnp.where(phase == 1, 1.0, jnp.where(phase == 3, -1.0, 0.0))
    blocks = []
    for spin in range(4):
        here = jnp.where(cols == spin, 1.0, 0.0)
        blocks.append(jnp.concatenate([here * real, here * imag], axis=1))
        blocks.append(jnp.concatenate([-here * imag, here * real], axis=1))
    return jnp.concatenate(blocks, axis=0)


def in_vmem(x):
    return pltpu.with_memory_space_constraint(x, VMEM)


VMEM_SPEC = pl.BlockSpec(memory_space=VMEM)
HBM_SPEC = pl.BlockSpec(memory_space=pltpu.MemorySpace.HBM)


def call(kernel, name, out_shape, *operands, specs=None):
    return pl.pallas_call(
        kernel,
        in_specs=specs or [VMEM_SPEC] * len(operands),
        out_specs=jax.tree.map(lambda _: VMEM_SPEC, out_shape),
        out_shape=out_shape,
        compiler_params=pltpu.CompilerParams(vmem_limit_bytes=8 << 20),
        name=name,
    )(*operands)


def local(left_modes, right_modes, gamma_cols, gamma_phase, dilution, time_pairs):
    left = jnp.transpose(left_modes, (0, 1, 2, 4, 3, 5))
    right = jnp.transpose(right_modes, (0, 1, 2, 4, 3, 5))
    dil = dilution.reshape(1, 64)

    partial, coef, spin_of = products(left, right, dil, gamma_cols.T, gamma_phase.T)
    partial = partial.reshape(16, 160, 128)
    parts = lax.all_to_all(partial, AXES, 0, 0, axis_index_groups=PLANES, tiled=True)
    plane = call(sum_planes_kernel, "sum_planes", pltpu.VMEM((320, 128), jnp.float32), in_vmem(parts.reshape(2560, 128)))
    parts = lax.all_to_all(plane.reshape(16, 1, 2560), AXES, 0, 0, axis_index_groups=COLUMNS, tiled=True)
    rows = call(
        combine_kernel,
        "combine",
        pltpu.VMEM((256, 128), jnp.float32),
        in_vmem(parts.reshape(320, 128)),
        in_vmem(coef),
        in_vmem(spin_of),
        in_vmem(time_pairs.T),
    )
    got = lax.all_to_all(rows.reshape(128, 2, 128), AXES, 0, 0, axis_index_groups=SAME_CORE, tiled=True)
    fields, traces = pl.pallas_call(
        finish_kernel,
        in_specs=[VMEM_SPEC],
        out_specs=[VMEM_SPEC, VMEM_SPEC],
        out_shape=[
            jax.ShapeDtypeStruct((1, 2, 2, 8, 128), jnp.float32),
            jax.ShapeDtypeStruct((4, 1, 2, 16), jnp.float32),
        ],
        name="finish",
    )(in_vmem(got.reshape(256, 128)))
    return (fields, jnp.swapaxes(traces, 2, 3))


def solution(mesh):
    return jax.shard_map(
        local,
        mesh=mesh,
        in_specs=(
            P(None, None, None, None, None, AXES),
            P(None, None, None, None, None, AXES),
            P(),
            P(),
            P(),
            P(),
        ),
        out_specs=(P("gz", None, None, ("gx", "gy"), None), P(None, "gz", None, None)),
        check_vma=False,
    )
```

```python
import jax
import jax.numpy as jnp
from jax import lax
from jax.experimental import pallas as pl
from jax.experimental.pallas import tpu as pltpu
from jax.sharding import PartitionSpec as P

AXES = ("gx", "gy", "gz")
EXACT = lax.Precision.HIGHEST
CHIPS = 128
ROWS = 20
VMEM = pltpu.MemorySpace.VMEM


def flat_index(chip, core):
    bit = [(chip >> k) & 1 for k in range(7)]
    return bit[6] * 128 + bit[4] * 64 + bit[3] * 32 + core * 16 + (chip & 3) * 4 + bit[2] * 2 + bit[5]


BLOCKS = [[flat_index(block * 4 + z, core) for block in range(32)] for z in range(4) for core in range(2)]
COLUMNS = [[flat_index(block * 4 + z, core) for core in range(2) for z in range(4)] for block in range(32)]
PARTNER = [(flat_index(chip, core), flat_index(chip, 1 - core)) for chip in range(CHIPS) for core in range(2)]
SAME_CORE = [sorted(flat_index(chip, core) for chip in range(CHIPS)) for core in range(2)]


def lane_iota(shape):
    return lax.broadcasted_iota(jnp.int32, shape, len(shape) - 1)


def row_iota(shape):
    return lax.broadcasted_iota(jnp.int32, shape, len(shape) - 2)


def place():
    gx, gy, gz = (lax.axis_index(name) for name in AXES)
    chip = (gx >> 1) * 64 + (gz & 1) * 32 + (gx & 1) * 16 + (gy >> 1) * 8 + ((gz >> 1) & 1) * 4 + (gz >> 2)
    return chip, gy & 1, gx * 4 + gy


def fill_pick(dil_ref, pick_ref):
    dilution = jnp.broadcast_to(jnp.concatenate([dil_ref[...], dil_ref[...]], axis=1), (128, 128))
    spin_of = jnp.transpose(dilution)[0:64, :]
    for spin in range(4):
        one = jnp.where(spin_of == spin, 1.0, 0.0).astype(jnp.bfloat16)
        pick_ref[spin] = jnp.concatenate([one] * 4, axis=1)


def fill_rows(right_ref, pick_ref, rows_ref):
    for part in range(2):
        for colour in range(3):
            at = (part * 3 + colour) * 512
            noise = None
            for spin in range(4):
                rows_ref[spin * 64 : spin * 64 + 64, at : at + 512] = right_ref[spin, part, colour, 0:64, :]
                term = right_ref[spin, part, colour, 64:128, :] * pick_ref[spin]
                noise = term if noise is None else noise + term
            rows_ref[256:320, at : at + 512] = noise


def add_tile(step, left_ref, rows_ref, out_ref):
    cols = []
    for part in range(2):
        for colour in range(3):
            pieces = []
            for tile in range(2):
                lines = slice(step * 32 + tile * 16, step * 32 + tile * 16 + 16)
                for spin in range(4):
                    pieces.append(left_ref[spin, part, colour, lines, :])
                for spin in range(4):
                    other = left_ref[spin, 1 - part, colour, lines, :]
                    pieces.append(-other if part == 0 else other)
            cols.append(jnp.concatenate(pieces, axis=0))
    prod = lax.dot_general(
        rows_ref[...],
        jnp.concatenate(cols, axis=1),
        (((1,), (1,)), ((), ())),
        preferred_element_type=jnp.float32,
    )
    low_i = lane_iota((8, 128)) & 15
    within = row_iota((8, 128)) ^ (low_i & 7)
    upper = low_i >= 8
    for tile in range(2):
        i_high = step * 2 + tile
        for block in range(20):
            first = prod[block * 16 : block * 16 + 8, tile * 128 : tile * 128 + 128]
            second = prod[block * 16 + 8 : block * 16 + 16, tile * 128 : tile * 128 + 128]
            j_high = block % 4 if block < 16 else block - 12
            start = (i_high ^ j_high) * (16 * ROWS) + block
            low_half = jnp.take_along_axis(jnp.where(upper, second, first), within, axis=0)
            high_half = jnp.take_along_axis(jnp.where(upper, first, second), within, axis=0)
            out_ref[pl.ds(start, 8, stride=ROWS), :] = low_half
            out_ref[pl.ds(start + 8 * ROWS, 8, stride=ROWS), :] = high_half


def away_kernel(
    left_ref, right_ref, dil_ref, cols_ref, phase_ref, out_ref, next_left_ref, next_right_ref, pick_ref, coef_ref, spin_ref,
    rows_ref, left_buf, right_buf, dil_buf, cols_buf, phase_buf, sems
):
    chip, core, _ = place()
    small = [
        pltpu.make_async_copy(dil_ref, dil_buf, sems.at[0]),
        pltpu.make_async_copy(cols_ref, cols_buf, sems.at[33]),
        pltpu.make_async_copy(phase_ref, phase_buf, sems.at[34]),
    ]
    copies = []
    for spin in range(4):
        for part in range(2):
            at = (spin, part)
            sem = sems.at[1 + spin * 2 + part]
            copies.append(pltpu.make_async_copy(right_ref.at[(1 - core,) + at], right_buf.at[at], sem))
    for spin in range(4):
        for part in range(2):
            at = (spin, part)
            sem = sems.at[9 + spin * 2 + part]
            copies.append(pltpu.make_async_copy(left_ref.at[(1 - core,) + at], left_buf.at[at], sem))
    next_copies = []
    for which, (source, target) in enumerate(((right_ref, next_right_ref), (left_ref, next_left_ref))):
        for spin in range(4):
            for part in range(2):
                at = (spin, part)
                sem = sems.at[17 + which * 8 + spin * 2 + part]
                next_copies.append(pltpu.make_async_copy(source.at[(core,) + at], target.at[at], sem))
    for copy in small + copies + next_copies:
        copy.start()
    for copy in small:
        copy.wait()
    fill_pick(dil_buf, pick_ref)
    coef_ref[...] = coefficients(cols_buf[...], phase_buf[...])
    dilution = jnp.broadcast_to(jnp.concatenate([dil_buf[...], dil_buf[...]], axis=1), (8, 128))
    spin_ref[...] = lane_pick(dilution, lane_iota((8, 128)) ^ (chip & 15))
    for copy in copies:
        copy.wait()
    fill_rows(right_buf, pick_ref, rows_ref)
    for step in range(4):
        add_tile(step, left_buf, rows_ref, out_ref)
    for copy in next_copies:
        copy.wait()


def home_kernel(left_ref, right_ref, pick_ref, out_ref, rows_ref):
    fill_rows(right_ref, pick_ref, rows_ref)
    for step in range(4):
        add_tile(step, left_ref, rows_ref, out_ref)


def products(left, right, dil, cols, phase):
    slot = (4, 2, 3, 128, 512)
    rows = pltpu.VMEM((320, 3072), jnp.bfloat16)
    whole = pltpu.VMEM((CHIPS * ROWS, 128), jnp.float32)
    away, next_left, next_right, pick, coef, spin_of = pl.pallas_call(
        away_kernel,
        in_specs=[HBM_SPEC] * 5,
        out_specs=[VMEM_SPEC] * 6,
        out_shape=[
            whole,
            pltpu.VMEM(slot, jnp.bfloat16),
            pltpu.VMEM(slot, jnp.bfloat16),
            pltpu.VMEM((4, 64, 512), jnp.bfloat16),
            pltpu.VMEM((32, 32), jnp.float32),
            pltpu.VMEM((8, 128), jnp.int32),
        ],
        scratch_shapes=[
            rows,
            pltpu.VMEM(slot, jnp.bfloat16),
            pltpu.VMEM(slot, jnp.bfloat16),
            pltpu.VMEM((1, 64), jnp.int32),
            pltpu.VMEM((4, 16), jnp.int32),
            pltpu.VMEM((4, 16), jnp.int32),
            pltpu.SemaphoreType.DMA((35,)),
        ],
        compiler_params=pltpu.CompilerParams(vmem_limit_bytes=16 << 20),
        name="away",
    )(*(pltpu.with_memory_space_constraint(x, pltpu.MemorySpace.HBM) for x in (left, right, dil, cols, phase)))
    arrived = lax.ppermute(away, AXES, PARTNER)
    home = pl.pallas_call(
        home_kernel,
        in_specs=[VMEM_SPEC] * 3,
        out_specs=VMEM_SPEC,
        out_shape=whole,
        scratch_shapes=[rows],
        compiler_params=pltpu.CompilerParams(vmem_limit_bytes=12 << 20),
        name="home",
    )(in_vmem(next_left), in_vmem(next_right), in_vmem(pick))
    return call(add_kernel, "add", whole, in_vmem(home), in_vmem(arrived)), coef, spin_of


def add_kernel(a_ref, b_ref, out_ref):
    out_ref[...] = a_ref[...] + b_ref[...]


def sum_blocks_kernel(parts_ref, out_ref):
    total = parts_ref[0:80, :]
    for k in range(1, 32):
        total = total + parts_ref[k * 80 : k * 80 + 80, :]
    out_ref[0:80, :] = total
    out_ref[80:160, :] = total


def dot_exact(a, b, dims):
    return lax.dot_general(a, b, (dims, ((), ())), precision=EXACT, preferred_element_type=jnp.float32)


def lane_pick(x, lanes):
    return jnp.take_along_axis(x, lanes, axis=1)


def combine_kernel(parts_ref, coef_ref, spin_ref, pairs_ref, out_ref):
    chip, core, _ = place()
    lane8 = lane_iota((8, 128))
    row8 = row_iota((8, 128))
    block = lane8 >> 4
    turn = ((block + row8) & 7) * 16 + (lane8 & 15)
    fall = (row8 - block) & 7
    back = ((row8 - block) & 7) * 16 + (lane8 & 15)
    spin_of = spin_ref[...]
    fields = []
    for time in range(2):
        total = parts_ref[time * 80 : time * 80 + ROWS, :]
        for z in range(1, 4):
            at = time * 80 + z * ROWS
            total = total + parts_ref[at : at + ROWS, :]
        terms = []
        for spin in range(4):
            x = jnp.concatenate([total[spin * 4 : spin * 4 + 4], total[16:20]], axis=0)
            x = lane_pick(jnp.take_along_axis(lane_pick(x, turn), fall, axis=0), back)
            keep = jnp.logical_or(lane8 < 64, spin_of == spin)
            terms.append(jnp.where(keep, x, 0.0))
        fields.append(dot_exact(coef_ref[...], jnp.concatenate(terms, axis=0), ((0,), (0,))))
    both = jnp.concatenate(fields, axis=0)
    lanes = lane_iota((64, 128))
    mirror = lane_pick(both, lanes ^ chip)
    cross = dot_exact(both, mirror, ((1,), (1,)))
    crossed = []
    for time in range(2):
        real = cross[time * 32 : time * 32 + 16]
        imag = cross[time * 32 + 16 : time * 32 + 32]
        for at in (0, 32):
            real_part = real[:, at : at + 16] - imag[:, at + 16 : at + 32]
            imag_part = real[:, at + 16 : at + 32] + imag[:, at : at + 16]
            crossed.append(jnp.concatenate([real_part, imag_part], axis=1))
    columns = []
    for pair in range(4):
        first = jnp.broadcast_to(pairs_ref[0:1, pair : pair + 1], (16, 32)) == 0
        second = jnp.broadcast_to(pairs_ref[1:2, pair : pair + 1], (16, 32)) == 0
        columns.append(
            jnp.where(first, jnp.where(second, crossed[0], crossed[1]), jnp.where(second, crossed[2], crossed[3]))
        )
    trace_rows = jnp.concatenate(columns, axis=1)
    ordered = lane_pick(both, ((lanes + 8 * core) & 127) ^ (chip & 112))
    lane = lane_iota((16, 128))
    for pair in range(8):
        rows = jnp.zeros((16, 128), jnp.float32)
        for k in range(4):
            moved = pltpu.roll(ordered[k * 16 : k * 16 + 16], (8 * k - 16 * pair) % 128, 1)
            rows = jnp.where((lane >> 3) == k, moved, rows)
        out_ref[pl.ds(pair * 32, 16, stride=2), :] = trace_rows
        out_ref[pl.ds(pair * 32 + 1, 16, stride=2), :] = rows


def finish_kernel(got_ref, fields_ref, traces_ref):
    _, _, block = place()
    row = row_iota((32, 128))
    pieces = []
    total = None
    for high in range(16):
        x_high, y_high, x_low, y_low = ((high >> k) & 1 for k in (3, 2, 1, 0))
        at = (x_high * 4 + x_low * 2 + y_low) * 32 + y_high * 2
        for odd in range(2):
            piece = got_ref[pl.ds(at + odd * 4, 4, stride=8), :]
            total = piece if total is None else total + piece
            pieces.append(got_ref[pl.ds(at + odd * 4 + 1, 4, stride=8), :])
    sums = jnp.sum(total, axis=0, keepdims=True)
    x = jnp.transpose(jnp.concatenate(pieces, axis=0))[0:32, :]
    x = lane_pick(x, lane_iota((32, 128)) ^ (block * 8 + (row & 7)))
    for time in range(2):
        for part in range(2):
            at = (time * 2 + part) * 8
            fields_ref[0, time, part] = x[at : at + 8]
    sums = sums / 128.0
    for pair in range(4):
        traces_ref[pair, 0, 0:1, :] = sums[:, pair * 32 : pair * 32 + 16]
        traces_ref[pair, 0, 1:2, :] = sums[:, pair * 32 + 16 : pair * 32 + 32]


def coefficients(cols, phase):
    real = jnp.where(phase == 0, 1.0, jnp.where(phase == 2, -1.0, 0.0))
    imag = jnp.where(phase == 1, 1.0, jnp.where(phase == 3, -1.0, 0.0))
    blocks = []
    for spin in range(4):
        here = jnp.where(cols == spin, 1.0, 0.0)
        blocks.append(jnp.concatenate([here * real, here * imag], axis=1))
        blocks.append(jnp.concatenate([-here * imag, here * real], axis=1))
    return jnp.concatenate(blocks, axis=0)


def in_vmem(x):
    return pltpu.with_memory_space_constraint(x, VMEM)


VMEM_SPEC = pl.BlockSpec(memory_space=VMEM)
HBM_SPEC = pl.BlockSpec(memory_space=pltpu.MemorySpace.HBM)


def call(kernel, name, out_shape, *operands, specs=None):
    return pl.pallas_call(
        kernel,
        in_specs=specs or [VMEM_SPEC] * len(operands),
        out_specs=jax.tree.map(lambda _: VMEM_SPEC, out_shape),
        out_shape=out_shape,
        compiler_params=pltpu.CompilerParams(vmem_limit_bytes=8 << 20),
        name=name,
    )(*operands)


def local(left_modes, right_modes, gamma_cols, gamma_phase, dilution, time_pairs):
    left = jnp.transpose(left_modes, (0, 1, 2, 4, 3, 5))
    right = jnp.transpose(right_modes, (0, 1, 2, 4, 3, 5))
    dil = dilution.reshape(1, 64)

    partial, coef, spin_of = products(left, right, dil, gamma_cols.T, gamma_phase.T)
    partial = partial.reshape(32, 80, 128)
    parts = lax.all_to_all(partial, AXES, 0, 0, axis_index_groups=BLOCKS, tiled=True)
    plane = call(sum_blocks_kernel, "sum_blocks", pltpu.VMEM((160, 128), jnp.float32), in_vmem(parts.reshape(2560, 128)))
    parts = lax.all_to_all(plane.reshape(8, 1, 2560), AXES, 0, 0, axis_index_groups=COLUMNS, tiled=True)
    rows = call(
        combine_kernel,
        "combine",
        pltpu.VMEM((256, 128), jnp.float32),
        in_vmem(parts.reshape(160, 128)),
        in_vmem(coef),
        in_vmem(spin_of),
        in_vmem(time_pairs.T),
    )
    got = lax.all_to_all(rows.reshape(128, 2, 128), AXES, 0, 0, axis_index_groups=SAME_CORE, tiled=True)
    fields, traces = pl.pallas_call(
        finish_kernel,
        in_specs=[VMEM_SPEC],
        out_specs=[VMEM_SPEC, VMEM_SPEC],
        out_shape=[
            jax.ShapeDtypeStruct((1, 2, 2, 8, 128), jnp.float32),
            jax.ShapeDtypeStruct((4, 1, 2, 16), jnp.float32),
        ],
        name="finish",
    )(in_vmem(got.reshape(256, 128)))
    return (fields, jnp.swapaxes(traces, 2, 3))


def solution(mesh):
    return jax.shard_map(
        local,
        mesh=mesh,
        in_specs=(
            P(None, None, None, None, None, AXES),
            P(None, None, None, None, None, AXES),
            P(),
            P(),
            P(),
            P(),
        ),
        out_specs=(P("gz", None, None, ("gx", "gy"), None), P(None, "gz", None, None)),
        check_vma=False,
    )
```

```python
import jax
import jax.numpy as jnp
from jax import lax
from jax.experimental import pallas as pl
from jax.experimental.pallas import tpu as pltpu
from jax.sharding import PartitionSpec as P

AXES = ("gx", "gy", "gz")
CHIPS = 128
ROWS = 20
VMEM = pltpu.MemorySpace.VMEM


def flat_index(chip, core):
    bit = [(chip >> k) & 1 for k in range(7)]
    return bit[6] * 128 + bit[4] * 64 + bit[3] * 32 + core * 16 + (chip & 3) * 4 + bit[2] * 2 + bit[5]


BLOCKS = [[flat_index(block * 4 + z, core) for block in range(32)] for z in range(4) for core in range(2)]
COLUMNS = [[flat_index(block * 4 + z, core) for core in range(2) for z in range(4)] for block in range(32)]
PARTNER = [(flat_index(chip, core), flat_index(chip, 1 - core)) for chip in range(CHIPS) for core in range(2)]
SAME_CORE = [sorted(flat_index(chip, core) for chip in range(CHIPS)) for core in range(2)]


def lane_iota(shape):
    return lax.broadcasted_iota(jnp.int32, shape, len(shape) - 1)


def row_iota(shape):
    return lax.broadcasted_iota(jnp.int32, shape, len(shape) - 2)


def place():
    gx, gy, gz = (lax.axis_index(name) for name in AXES)
    chip = (gx >> 1) * 64 + (gz & 1) * 32 + (gx & 1) * 16 + (gy >> 1) * 8 + ((gz >> 1) & 1) * 4 + (gz >> 2)
    return chip, gy & 1, gx * 4 + gy


def fill_pick(dil_ref, pick_ref):
    dilution = jnp.broadcast_to(jnp.concatenate([dil_ref[...], dil_ref[...]], axis=1), (128, 128))
    spin_of = jnp.transpose(dilution)[0:64, :]
    for spin in range(4):
        one = jnp.where(spin_of == spin, 1.0, 0.0).astype(jnp.bfloat16)
        pick_ref[spin] = jnp.concatenate([one] * 4, axis=1)


def fill_rows(right_ref, pick_ref, rows_ref):
    for part in range(2):
        for colour in range(3):
            at = (part * 3 + colour) * 512
            noise = None
            for spin in range(4):
                rows_ref[spin * 64 : spin * 64 + 64, at : at + 512] = right_ref[spin, part, colour, 0:64, :]
                term = right_ref[spin, part, colour, 64:128, :] * pick_ref[spin]
                noise = term if noise is None else noise + term
            rows_ref[256:320, at : at + 512] = noise


def add_tile(step, left_ref, rows_ref, out_ref):
    cols = []
    for part in range(2):
        for colour in range(3):
            pieces = []
            for tile in range(2):
                lines = slice(step * 32 + tile * 16, step * 32 + tile * 16 + 16)
                for spin in range(4):
                    pieces.append(left_ref[spin, part, colour, lines, :])
                for spin in range(4):
                    other = left_ref[spin, 1 - part, colour, lines, :]
                    pieces.append(-other if part == 0 else other)
            cols.append(jnp.concatenate(pieces, axis=0))
    prod = lax.dot_general(
        rows_ref[...],
        jnp.concatenate(cols, axis=1),
        (((1,), (1,)), ((), ())),
        preferred_element_type=jnp.float32,
    )
    low_i = lane_iota((8, 128)) & 15
    within = row_iota((8, 128)) ^ (low_i & 7)
    upper = low_i >= 8
    for tile in range(2):
        i_high = step * 2 + tile
        for block in range(20):
            first = prod[block * 16 : block * 16 + 8, tile * 128 : tile * 128 + 128]
            second = prod[block * 16 + 8 : block * 16 + 16, tile * 128 : tile * 128 + 128]
            j_high = block % 4 if block < 16 else block - 12
            start = (i_high ^ j_high) * (16 * ROWS) + block
            low_half = jnp.take_along_axis(jnp.where(upper, second, first), within, axis=0)
            high_half = jnp.take_along_axis(jnp.where(upper, first, second), within, axis=0)
            out_ref[pl.ds(start, 8, stride=ROWS), :] = low_half
            out_ref[pl.ds(start + 8 * ROWS, 8, stride=ROWS), :] = high_half


def away_kernel(
    left_ref, right_ref, dil_ref, cols_ref, phase_ref, out_ref, next_left_ref, next_right_ref, pick_ref, coef_ref, spin_ref,
    rows_ref, left_buf, right_buf, dil_buf, cols_buf, phase_buf, sems
):
    chip, core, _ = place()
    small = [
        pltpu.make_async_copy(dil_ref, dil_buf, sems.at[0]),
        pltpu.make_async_copy(cols_ref, cols_buf, sems.at[33]),
        pltpu.make_async_copy(phase_ref, phase_buf, sems.at[34]),
    ]
    copies = []
    for spin in range(4):
        for part in range(2):
            at = (spin, part)
            sem = sems.at[1 + spin * 2 + part]
            copies.append(pltpu.make_async_copy(right_ref.at[(1 - core,) + at], right_buf.at[at], sem))
    for spin in range(4):
        for part in range(2):
            at = (spin, part)
            sem = sems.at[9 + spin * 2 + part]
            copies.append(pltpu.make_async_copy(left_ref.at[(1 - core,) + at], left_buf.at[at], sem))
    next_copies = []
    for which, (source, target) in enumerate(((right_ref, next_right_ref), (left_ref, next_left_ref))):
        for spin in range(4):
            for part in range(2):
                at = (spin, part)
                sem = sems.at[17 + which * 8 + spin * 2 + part]
                next_copies.append(pltpu.make_async_copy(source.at[(core,) + at], target.at[at], sem))
    for copy in small + copies + next_copies:
        copy.start()
    for copy in small:
        copy.wait()
    fill_pick(dil_buf, pick_ref)
    coef_ref[...] = coefficients(cols_buf[...], phase_buf[...])
    dilution = jnp.broadcast_to(jnp.concatenate([dil_buf[...], dil_buf[...]], axis=1), (8, 128))
    spin_ref[...] = lane_pick(dilution, lane_iota((8, 128)) ^ (chip & 15))
    for copy in copies:
        copy.wait()
    fill_rows(right_buf, pick_ref, rows_ref)
    for step in range(4):
        add_tile(step, left_buf, rows_ref, out_ref)
    for copy in next_copies:
        copy.wait()


def home_kernel(left_ref, right_ref, pick_ref, out_ref, rows_ref):
    fill_rows(right_ref, pick_ref, rows_ref)
    for step in range(4):
        add_tile(step, left_ref, rows_ref, out_ref)


def products(left, right, dil, cols, phase):
    slot = (4, 2, 3, 128, 512)
    rows = pltpu.VMEM((320, 3072), jnp.bfloat16)
    whole = pltpu.VMEM((CHIPS * ROWS, 128), jnp.float32)
    away, next_left, next_right, pick, coef, spin_of = pl.pallas_call(
        away_kernel,
        in_specs=[HBM_SPEC] * 5,
        out_specs=[VMEM_SPEC] * 6,
        out_shape=[
            whole,
            pltpu.VMEM(slot, jnp.bfloat16),
            pltpu.VMEM(slot, jnp.bfloat16),
            pltpu.VMEM((4, 64, 512), jnp.bfloat16),
            pltpu.VMEM((32, 32), jnp.float32),
            pltpu.VMEM((8, 128), jnp.int32),
        ],
        scratch_shapes=[
            rows,
            pltpu.VMEM(slot, jnp.bfloat16),
            pltpu.VMEM(slot, jnp.bfloat16),
            pltpu.VMEM((1, 64), jnp.int32),
            pltpu.VMEM((4, 16), jnp.int32),
            pltpu.VMEM((4, 16), jnp.int32),
            pltpu.SemaphoreType.DMA((35,)),
        ],
        compiler_params=pltpu.CompilerParams(vmem_limit_bytes=16 << 20),
        name="away",
    )(*(pltpu.with_memory_space_constraint(x, pltpu.MemorySpace.HBM) for x in (left, right, dil, cols, phase)))
    arrived = lax.ppermute(away, AXES, PARTNER)
    home = pl.pallas_call(
        home_kernel,
        in_specs=[VMEM_SPEC] * 3,
        out_specs=VMEM_SPEC,
        out_shape=whole,
        scratch_shapes=[rows],
        compiler_params=pltpu.CompilerParams(vmem_limit_bytes=12 << 20),
        name="home",
    )(in_vmem(next_left), in_vmem(next_right), in_vmem(pick))
    return call(add_kernel, "add", whole, in_vmem(home), in_vmem(arrived)), coef, spin_of


def add_kernel(a_ref, b_ref, out_ref):
    out_ref[...] = a_ref[...] + b_ref[...]


def sum_blocks_kernel(parts_ref, out_ref):
    total = parts_ref[0:80, :]
    for k in range(1, 32):
        total = total + parts_ref[k * 80 : k * 80 + 80, :]
    out_ref[0:80, :] = total
    out_ref[80:160, :] = total


def split(x):
    high = x.astype(jnp.bfloat16)
    rest = x - high.astype(jnp.float32)
    middle = rest.astype(jnp.bfloat16)
    return high, middle, (rest - middle.astype(jnp.float32)).astype(jnp.bfloat16)


def dot(a, b, dims):
    return lax.dot_general(a, b, (dims, ((), ())), preferred_element_type=jnp.float32)


def lane_pick(x, lanes):
    return jnp.take_along_axis(x, lanes, axis=1)


def combine_kernel(parts_ref, coef_ref, spin_ref, pairs_ref, out_ref):
    chip, core, _ = place()
    lane8 = lane_iota((8, 128))
    row8 = row_iota((8, 128))
    block = lane8 >> 4
    turn = ((block + row8) & 7) * 16 + (lane8 & 15)
    fall = (row8 - block) & 7
    back = ((row8 - block) & 7) * 16 + (lane8 & 15)
    spin_of = spin_ref[...]
    coef = jnp.concatenate([coef_ref[...].astype(jnp.bfloat16)] * 3, axis=0)
    fields = []
    for time in range(2):
        total = parts_ref[time * 80 : time * 80 + ROWS, :]
        for z in range(1, 4):
            at = time * 80 + z * ROWS
            total = total + parts_ref[at : at + ROWS, :]
        terms = []
        for spin in range(4):
            x = jnp.concatenate([total[spin * 4 : spin * 4 + 4], total[16:20]], axis=0)
            x = lane_pick(jnp.take_along_axis(lane_pick(x, turn), fall, axis=0), back)
            keep = jnp.logical_or(lane8 < 64, spin_of == spin)
            terms.append(jnp.where(keep, x, 0.0))
        parts = jnp.concatenate(split(jnp.concatenate(terms, axis=0)), axis=0)
        fields.append(dot(coef, parts, ((0,), (0,))))
    both = jnp.concatenate(fields, axis=0)
    lanes = lane_iota((64, 128))
    mirror = lane_pick(both, lanes ^ chip)
    a_high, a_middle, a_low = split(both)
    b_high, b_middle, b_low = split(mirror)
    cross = dot(
        jnp.concatenate([a_low, a_high, a_middle, a_middle, a_high, a_high], axis=1),
        jnp.concatenate([b_high, b_low, b_middle, b_high, b_middle, b_high], axis=1),
        ((1,), (1,)),
    )
    crossed = []
    for time in range(2):
        real = cross[time * 32 : time * 32 + 16]
        imag = cross[time * 32 + 16 : time * 32 + 32]
        for at in (0, 32):
            real_part = real[:, at : at + 16] - imag[:, at + 16 : at + 32]
            imag_part = real[:, at + 16 : at + 32] + imag[:, at : at + 16]
            crossed.append(jnp.concatenate([real_part, imag_part], axis=1))
    columns = []
    for pair in range(4):
        first = jnp.broadcast_to(pairs_ref[0:1, pair : pair + 1], (16, 32)) == 0
        second = jnp.broadcast_to(pairs_ref[1:2, pair : pair + 1], (16, 32)) == 0
        columns.append(
            jnp.where(first, jnp.where(second, crossed[0], crossed[1]), jnp.where(second, crossed[2], crossed[3]))
        )
    trace_rows = jnp.concatenate(columns, axis=1)
    ordered = lane_pick(both, ((lanes + 8 * core) & 127) ^ (chip & 112))
    lane = lane_iota((16, 128))
    for pair in range(8):
        rows = jnp.zeros((16, 128), jnp.float32)
        for k in range(4):
            moved = pltpu.roll(ordered[k * 16 : k * 16 + 16], (8 * k - 16 * pair) % 128, 1)
            rows = jnp.where((lane >> 3) == k, moved, rows)
        out_ref[pl.ds(pair * 32, 16, stride=2), :] = trace_rows
        out_ref[pl.ds(pair * 32 + 1, 16, stride=2), :] = rows


def finish_kernel(got_ref, fields_ref, traces_ref):
    _, _, block = place()
    row = row_iota((32, 128))
    pieces = []
    total = None
    for high in range(16):
        x_high, y_high, x_low, y_low = ((high >> k) & 1 for k in (3, 2, 1, 0))
        at = (x_high * 4 + x_low * 2 + y_low) * 32 + y_high * 2
        for odd in range(2):
            piece = got_ref[pl.ds(at + odd * 4, 4, stride=8), :]
            total = piece if total is None else total + piece
            pieces.append(got_ref[pl.ds(at + odd * 4 + 1, 4, stride=8), :])
    sums = jnp.sum(total, axis=0, keepdims=True)
    x = jnp.transpose(jnp.concatenate(pieces, axis=0))[0:32, :]
    x = lane_pick(x, lane_iota((32, 128)) ^ (block * 8 + (row & 7)))
    for time in range(2):
        for part in range(2):
            at = (time * 2 + part) * 8
            fields_ref[0, time, part] = x[at : at + 8]
    sums = sums / 128.0
    for pair in range(4):
        traces_ref[pair, 0, 0:1, :] = sums[:, pair * 32 : pair * 32 + 16]
        traces_ref[pair, 0, 1:2, :] = sums[:, pair * 32 + 16 : pair * 32 + 32]


def coefficients(cols, phase):
    real = jnp.where(phase == 0, 1.0, jnp.where(phase == 2, -1.0, 0.0))
    imag = jnp.where(phase == 1, 1.0, jnp.where(phase == 3, -1.0, 0.0))
    blocks = []
    for spin in range(4):
        here = jnp.where(cols == spin, 1.0, 0.0)
        blocks.append(jnp.concatenate([here * real, here * imag], axis=1))
        blocks.append(jnp.concatenate([-here * imag, here * real], axis=1))
    return jnp.concatenate(blocks, axis=0)


def in_vmem(x):
    return pltpu.with_memory_space_constraint(x, VMEM)


VMEM_SPEC = pl.BlockSpec(memory_space=VMEM)
HBM_SPEC = pl.BlockSpec(memory_space=pltpu.MemorySpace.HBM)


def call(kernel, name, out_shape, *operands, specs=None):
    return pl.pallas_call(
        kernel,
        in_specs=specs or [VMEM_SPEC] * len(operands),
        out_specs=jax.tree.map(lambda _: VMEM_SPEC, out_shape),
        out_shape=out_shape,
        compiler_params=pltpu.CompilerParams(vmem_limit_bytes=8 << 20),
        name=name,
    )(*operands)


def local(left_modes, right_modes, gamma_cols, gamma_phase, dilution, time_pairs):
    left = jnp.transpose(left_modes, (0, 1, 2, 4, 3, 5))
    right = jnp.transpose(right_modes, (0, 1, 2, 4, 3, 5))
    dil = dilution.reshape(1, 64)

    partial, coef, spin_of = products(left, right, dil, gamma_cols.T, gamma_phase.T)
    partial = partial.reshape(32, 80, 128)
    parts = lax.all_to_all(partial, AXES, 0, 0, axis_index_groups=BLOCKS, tiled=True)
    plane = call(sum_blocks_kernel, "sum_blocks", pltpu.VMEM((160, 128), jnp.float32), in_vmem(parts.reshape(2560, 128)))
    parts = lax.all_to_all(plane.reshape(8, 1, 2560), AXES, 0, 0, axis_index_groups=COLUMNS, tiled=True)
    rows = call(
        combine_kernel,
        "combine",
        pltpu.VMEM((256, 128), jnp.float32),
        in_vmem(parts.reshape(160, 128)),
        in_vmem(coef),
        in_vmem(spin_of),
        in_vmem(time_pairs.T),
    )
    got = lax.all_to_all(rows.reshape(128, 2, 128), AXES, 0, 0, axis_index_groups=SAME_CORE, tiled=True)
    fields, traces = pl.pallas_call(
        finish_kernel,
        in_specs=[VMEM_SPEC],
        out_specs=[VMEM_SPEC, VMEM_SPEC],
        out_shape=[
            jax.ShapeDtypeStruct((1, 2, 2, 8, 128), jnp.float32),
            jax.ShapeDtypeStruct((4, 1, 2, 16), jnp.float32),
        ],
        name="finish",
    )(in_vmem(got.reshape(256, 128)))
    return (fields, jnp.swapaxes(traces, 2, 3))


def solution(mesh):
    return jax.shard_map(
        local,
        mesh=mesh,
        in_specs=(
            P(None, None, None, None, None, AXES),
            P(None, None, None, None, None, AXES),
            P(),
            P(),
            P(),
            P(),
        ),
        out_specs=(P("gz", None, None, ("gx", "gy"), None), P(None, "gz", None, None)),
        check_vma=False,
    )
```
